32 devices in a mesh: row: 4 (over z), col: 4 (over x, core), ch: 2 (over y).
Axes of the slice: x: 2, y: 2, z: 4, core: 2. Of those that a mesh axis runs over, the one named last changes fastest.
Arguments:
- image_tokens: bfloat16 [64, 1024, 128], P(('row', 'ch'), 'col'), may hold values from -61 to 61
- labels: int32 [64, 1024], P(('row', 'ch'), 'col'), may hold values from 0 to 2
- rel_index: int32 [64, 64], replicated, may hold values from 0 to 224
- norm_gain: float32 [2, 2, 128], replicated, may hold values from 0.25 to 1.75
- norm_shift: float32 [2, 2, 128], replicated, may hold values from -1.5 to 1.5
- qkv_weight: bfloat16 [2, 3, 128, 128], P(None, None, None, 'ch'), may hold values from -5 to 5
- qkv_bias: float32 [2, 3, 128], P(None, None, 'ch'), may hold values from -1.5 to 1.5
- bias_table: float32 [2, 225, 4], P(None, None, 'ch'), may hold values from -4 to 4
- proj_weight: bfloat16 [2, 128, 128], P(None, 'ch'), may hold values from -0.5 to 0.5
- proj_bias: float32 [2, 128], replicated, may hold values from -1.5 to 1.5
- fc1_weight: bfloat16 [2, 128, 512], P(None, None, 'ch'), may hold values from -0.5 to 0.5
- fc1_bias: float32 [2, 512], P(None, 'ch'), may hold values from -2.5 to 2.5
- fc2_weight: bfloat16 [2, 512, 128], P(None, 'ch'), may hold values from -0.25 to 0.25
- fc2_bias: float32 [2, 128], replicated, may hold values from -1.5 to 1.5
Outputs:
- encoded: bfloat16 [64, 1024, 128], P(('row', 'ch'), 'col')
The draws below stay inside these ranges and needn't reach their ends.
All inputs are finite; a program needn't handle non-finite values.
Results may differ from the reference program's by a relative error of at most 0.014.
Values may be sent and summed in bfloat16 or wider, within the bound.
A program may use at most 128 MiB of HBM per device.

```python
import jax
import jax.numpy as jnp
from jax import lax

C = 128
HEADS = 4
MLP_WIDTH = 512
WIN = 8
SHIFT = 4
TABLE = 225
BLOCKS = 2
KINDS = 3
IMG_ROWS = 64
IMG_COLS = 1024


def draw_image_tokens(key, part):
    base_key = jax.random.fold_in(key, 11)
    values = jnp.clip(jax.random.normal(base_key, (IMG_ROWS, IMG_COLS, C), jnp.float32), -6.0, 6.0)
    return values.astype(jnp.bfloat16)


def draw_qkv_weight(key, part):
    noise_key = jax.random.fold_in(key, 21)
    noise = jnp.clip(jax.random.normal(noise_key, (BLOCKS, 3, C, C), jnp.float32), -4.0, 4.0) * C ** (-0.5)
    return noise.astype(jnp.bfloat16)


def place_ends(values, rng, smallest, high):
    dims = values.shape
    spot = [jax.random.randint(jax.random.fold_in(rng, axis), (), 0, dims[axis]) for axis in range(len(dims))]
    values = values.at[tuple(spot)].set(smallest)
    longest = dims.index(max(dims))
    spot[longest] = (spot[longest] + 1) % dims[longest]
    return values.at[tuple(spot)].set(high)


def steps_of(own_key, extent, shards, low, top_value):
    loudness = 1.0
    for dim, shards_of in shards:
        draws = jax.random.uniform(jax.random.fold_in(jax.random.fold_in(own_key, 6), dim), (shards_of,), jnp.float32, low / len(shards), top_value / len(shards))
        loudness = loudness * jnp.repeat(jnp.exp(draws), extent[dim] // shards_of).reshape((-1,) + (1,) * (len(extent) - 1 - dim))
    return loudness


def scatter_about(rng, extent, scale, bound, shards=(), held_as=jnp.bfloat16):
    drawn = scale * jax.random.normal(rng, extent, jnp.float32)
    if shards:
        drawn = drawn * steps_of(rng, extent, shards, -0.22, 0.18)
    return jnp.clip(drawn, -bound, bound).astype(held_as)


def setup_inputs(seed: int = 0) -> dict:
    arg_keys = jax.random.split(jax.random.key(seed), 15)
    image_tokens = draw_image_tokens(jax.random.fold_in(arg_keys[14], 71), 0)
    labels = place_ends(jax.random.randint(arg_keys[1], (IMG_ROWS, IMG_COLS), 0, KINDS), jax.random.fold_in(arg_keys[1], 1), 0, KINDS - 1).astype(jnp.int32)
    rel_index = place_ends(jax.random.randint(arg_keys[2], (WIN * WIN, WIN * WIN), 0, TABLE), jax.random.fold_in(arg_keys[2], 1), 0, TABLE - 1).astype(jnp.int32)
    norm_gain = jnp.clip(1.0 + 0.15 * jax.random.normal(arg_keys[3], (BLOCKS, 2, C), jnp.float32), 0.25, 1.75)
    norm_shift = scatter_about(arg_keys[4], (BLOCKS, 2, C), 0.3, 1.5, (), jnp.float32)
    qkv_weight = draw_qkv_weight(jax.random.fold_in(arg_keys[14], 71), 0)
    qkv_bias = scatter_about(arg_keys[6], (BLOCKS, 3, C), 0.3, 1.5, ((2, 2),), jnp.float32)
    bias_table = scatter_about(arg_keys[7], (BLOCKS, TABLE, HEADS), 1.0, 4.0, ((2, 2),), jnp.float32)
    proj_weight = scatter_about(arg_keys[8], (BLOCKS, C, C), C ** -0.5, 0.5, ((1, 2),))
    proj_bias = scatter_about(arg_keys[9], (BLOCKS, C), 0.3, 1.5, (), jnp.float32)
    fc1_weight = scatter_about(arg_keys[10], (BLOCKS, C, MLP_WIDTH), C ** -0.5, 0.5, ((2, 2),))
    fc1_bias = scatter_about(arg_keys[11], (BLOCKS, MLP_WIDTH), 0.5, 2.5, ((1, 2),), jnp.float32)
    fc2_weight = scatter_about(arg_keys[12], (BLOCKS, MLP_WIDTH, C), MLP_WIDTH ** -0.5, 0.25, ((1, 2),))
    fc2_bias = scatter_about(arg_keys[13], (BLOCKS, C), 0.3, 1.5, (), jnp.float32)
    return {"image_tokens": image_tokens, "labels": labels, "rel_index": rel_index, "norm_gain": norm_gain, "norm_shift": norm_shift, "qkv_weight": qkv_weight, "qkv_bias": qkv_bias, "bias_table": bias_table, "proj_weight": proj_weight, "proj_bias": proj_bias, "fc1_weight": fc1_weight, "fc1_bias": fc1_bias, "fc2_weight": fc2_weight, "fc2_bias": fc2_bias}


EPS = 1e-05

def layer_norm(values, gain, offset):
    widened = values.astype(jnp.float32)
    center = widened - lax.optimization_barrier(jnp.mean(widened, axis=-1, keepdims=True))
    spread = lax.optimization_barrier(jnp.mean(center * center, axis=-1, keepdims=True))
    return (center * lax.rsqrt(spread + EPS) * gain + offset).astype(jnp.bfloat16)

def position_bias(rel_index, table):
    entries = table.shape[0]
    onehot = (rel_index.reshape(-1, 1) == jnp.arange(entries, dtype=jnp.int32)[None, :]).astype(jnp.float32)
    picked = jnp.dot(onehot, table, precision=lax.Precision.HIGHEST, preferred_element_type=jnp.float32)
    length = rel_index.shape[0]
    return picked.T.reshape(table.shape[1], length, length)

def window_attention(triple, region, bias):
    rows, cols = (triple.shape[0], triple.shape[1])
    width = triple.shape[3]
    heads = bias.shape[0]
    depth = width // heads
    across = rows // WIN
    along = cols // WIN
    grid = triple.reshape(across, WIN, along, WIN, 3, heads, depth)
    grid = grid.transpose(0, 2, 4, 5, 1, 3, 6).reshape(across, along, 3, heads, WIN * WIN, depth)
    grid = grid.astype(jnp.float32)
    scores = jnp.einsum('abhpd,abhqd->abhpq', grid[:, :, 0], grid[:, :, 1])
    scores = scores * depth ** (-0.5) + bias
    if region is not None:
        window_ids = region.reshape(across, WIN, along, WIN).transpose(0, 2, 1, 3).reshape(across, along, WIN * WIN)
        allowed = window_ids[:, :, :, None] == window_ids[:, :, None, :]
        scores = jnp.where(allowed[:, :, None], scores, -jnp.inf)
    highest = lax.optimization_barrier(jnp.max(scores, axis=-1, keepdims=True))
    raised = jnp.exp(scores - highest)
    weights = (raised / lax.optimization_barrier(jnp.sum(raised, axis=-1, keepdims=True))).astype(jnp.bfloat16)
    mixed = jnp.einsum('abhpq,abhqd->abhpd', weights.astype(jnp.float32), grid[:, :, 2])
    mixed = mixed.astype(jnp.bfloat16).reshape(across, along, heads, WIN, WIN, depth)
    return mixed.transpose(0, 3, 1, 4, 2, 5).reshape(rows, cols, width)

def attend_image(triple, region, bias, offset):
    rolled = jnp.roll(triple, (-offset, -offset), axis=(0, 1))
    bands = rolled.reshape(IMG_ROWS // WIN, WIN, IMG_COLS, 3, C)
    if region is None:
        result = lax.map(lambda band: window_attention(band, None, bias), bands)
    else:
        region_bands = jnp.roll(region, (-offset, -offset), axis=(0, 1)).reshape(IMG_ROWS // WIN, WIN, IMG_COLS)
        result = lax.map(lambda pair: window_attention(pair[0], pair[1], bias), (bands, region_bands))
    result = result.reshape(IMG_ROWS, IMG_COLS, C)
    return jnp.roll(result, (offset, offset), axis=(0, 1))

def swin_block(tokens, block, region, offset, norm_gain, norm_shift, qkv_weight, qkv_bias, bias_table, proj_weight, proj_bias, fc1_weight, fc1_bias, fc2_weight, fc2_bias, rel_index):
    normed = layer_norm(tokens, norm_gain[block, 0], norm_shift[block, 0])
    stacked = qkv_weight[block].transpose(1, 0, 2).reshape(C, 3 * C)
    triple = jnp.dot(normed.reshape(-1, C), stacked, preferred_element_type=jnp.float32)
    triple = (triple.reshape(IMG_ROWS, IMG_COLS, 3, C) + qkv_bias[block]).astype(jnp.bfloat16)
    bias = position_bias(rel_index, bias_table[block])
    attended = attend_image(triple, region, bias, offset)
    mixed = jnp.dot(attended.reshape(-1, C), proj_weight[block], preferred_element_type=jnp.float32)
    middle = (tokens.astype(jnp.float32) + mixed.reshape(IMG_ROWS, IMG_COLS, C) + proj_bias[block]).astype(jnp.bfloat16)

    def feed(band):
        normed_two = layer_norm(band, norm_gain[block, 1], norm_shift[block, 1])
        inner = jnp.dot(normed_two.reshape(-1, C), fc1_weight[block], preferred_element_type=jnp.float32)
        hidden = jax.nn.gelu(inner + fc1_bias[block], approximate=False).astype(jnp.bfloat16)
        outer = jnp.dot(hidden, fc2_weight[block], preferred_element_type=jnp.float32).reshape(band.shape)
        return (band.astype(jnp.float32) + outer + fc2_bias[block]).astype(jnp.bfloat16)
    result = lax.map(feed, middle.reshape(IMG_ROWS // WIN, WIN, IMG_COLS, C))
    return result.reshape(IMG_ROWS, IMG_COLS, C)

def reference(image_tokens, labels, rel_index, norm_gain, norm_shift, qkv_weight, qkv_bias, bias_table, proj_weight, proj_bias, fc1_weight, fc1_bias, fc2_weight, fc2_bias):
    grid_rows = jnp.arange(IMG_ROWS, dtype=jnp.int32)
    grid_cols = jnp.arange(IMG_COLS, dtype=jnp.int32)
    region = labels * 4 + (grid_rows < SHIFT).astype(jnp.int32)[:, None] * 2 + (grid_cols < SHIFT).astype(jnp.int32)[None, :]
    current = image_tokens
    for block in range(BLOCKS):
        if block % 2 == 1:
            current = swin_block(current, block, region, SHIFT, norm_gain, norm_shift, qkv_weight, qkv_bias, bias_table, proj_weight, proj_bias, fc1_weight, fc1_bias, fc2_weight, fc2_bias, rel_index)
        else:
            current = swin_block(current, block, None, 0, norm_gain, norm_shift, qkv_weight, qkv_bias, bias_table, proj_weight, proj_bias, fc1_weight, fc1_bias, fc2_weight, fc2_bias, rel_index)
    return current
```

```python
import functools

import jax
import jax.numpy as jnp
from jax import lax
from jax.experimental import pallas as pl
from jax.experimental.pallas import tpu as pltpu
from jax.sharding import PartitionSpec as P

WIN = 8
SHIFT = 4
BLOCKS = 2
EPS = 1e-05
FAR = -1e30
LOG2E = 1.4426950408889634
MOST = 8
bf16 = jnp.bfloat16
f32 = jnp.float32
i32 = jnp.int32
KEYS = WIN * WIN
PART = SHIFT * SHIFT


def dot(a, b):
    return jnp.dot(a, b, preferred_element_type=f32)


def dot_t(a, b):
    return lax.dot_general(a, b, (((1,), (1,)), ((), ())), preferred_element_type=f32)


def layer_norm(x, gain, offset):
    center = x - jnp.mean(x, axis=-1, keepdims=True)
    spread = jnp.mean(center * center, axis=-1, keepdims=True)
    return (center * lax.rsqrt(spread + EPS) * gain + offset).astype(bf16)


def rows_of(x):
    return x.reshape(x.shape[0] * x.shape[1], x.shape[2])


def swap_halves(e, o):
    low = lax.broadcasted_iota(i32, e.shape, 1) < SHIFT
    return jnp.where(low, e, pltpu.roll(o, SHIFT, 1)), jnp.where(low, pltpu.roll(e, SHIFT, 1), o)


def quads(x):
    rows, wide, width = x.shape
    g = wide // WIN
    pairs = []
    for r in range(0, rows, 2):
        pairs.append(swap_halves(x[r].reshape(g, WIN, width), x[r + 1].reshape(g, WIN, width)))
    parts = []
    for w in range(g):
        for h in range(0, rows // 2, 2):
            parts += [pairs[h + i][s][w] for s in (0, 1) for i in (0, 1)]
    return jnp.concatenate(parts, axis=0)


def place_of(t):
    q, i = t >> 4, t & 15
    return SHIFT * (q >> 1) + (i >> 2), SHIFT * (q & 1) + (i & 3)


def head_mask(heads, keys, width):
    depth = width // heads
    row = lax.broadcasted_iota(i32, (heads * keys, width), 0) // keys
    col = lax.broadcasted_iota(i32, (heads * keys, width), 1) // depth
    return (row == col).astype(f32).astype(bf16)


def scores_of(triple, hmask, heads):
    width = triple.shape[1] // 3
    out = []
    for w in range(0, triple.shape[0], KEYS):
        q, k = triple[w : w + KEYS, :width], triple[w : w + KEYS, width : 2 * width]
        out.append(dot_t(q, jnp.concatenate([k] * heads, axis=0) * hmask))
    return out


def weigh(scores, bias, masks):
    low = lax.broadcasted_iota(i32, (KEYS, 128), 1) < KEYS
    weights = []
    for w, s in enumerate(scores):
        parts = []
        for c in range(0, s.shape[1], 128):
            t = s[:, c : c + 128] + bias[:, c : c + 128]
            if masks is not None:
                t = jnp.where(masks[w], t, FAR)
            u = t.astype(bf16)
            first = jnp.max(jnp.where(low, u, bf16(-jnp.inf)), axis=-1, keepdims=True)
            second = jnp.max(jnp.where(low, bf16(-jnp.inf), u), axis=-1, keepdims=True)
            parts.append(jnp.exp2(t - jnp.where(low, first, second).astype(f32)))
        weights.append(jnp.concatenate(parts, axis=1).astype(bf16))
    return weights


def blend(weights, triple, hmask, heads):
    width = triple.shape[1] // 3
    outs = []
    for w, p in enumerate(weights):
        v = triple[w * KEYS : (w + 1) * KEYS, 2 * width :]
        o = dot(p, jnp.concatenate([jnp.concatenate([v] * heads, axis=0) * hmask, hmask], axis=1))
        outs.append((o[:, :width] / o[:, width:]).astype(bf16))
    return outs


def pipeline(tasks, depth):
    for task in tasks:
        for stage in task:
            if stage is not None:
                stage()


def fused(
    heads, group,
    x_h, lab_h, rel_h, gain_h, shift_h, qkvw_h, qkvb_h, table_h, projw_h, projb_h, fc1w_h, fc1b_h, fc2w_h, fc2b_h,
    o_ref,
    x_v, lab, rel, gain, shift, table, proj_b, fc2_b,
    qkv, proj, fc1, fc2, tab_all, qb_all, f1b_all, qb, f1b, bias, lab3, rt, ru,
    xq, nq, att, x1, below, yr, yt, yo,
    in_sem, ssend, srecv, wsend, wrecv, rsend, rrecv, lsend, lrecv, hsend, hrecv, esend, erecv,
    osend, orecv, fsend, frecv,
):
    rows, cols, width = x_v.shape
    nwin = cols // WIN
    chunks = nwin // group
    n = lax.axis_size("ch")
    nrow, ncol = lax.axis_size("row"), lax.axis_size("col")
    row, col, ch = lax.axis_index("row"), lax.axis_index("col"), lax.axis_index("ch")
    ring = row * n + ch
    total = nrow * n

    def at(dr, dc):
        p = lax.rem(ring + dr + total, total)
        return (p // n, lax.rem(col + dc + ncol, ncol), lax.rem(p, n))

    around = [(-1, 0), (0, -1), (-1, -1), (1, 0), (0, 1), (1, 1)]
    peers = [(row, col, lax.rem(ch + d, n)) for d in range(1, n)]
    mate = (row, col + 1 - 2 * lax.rem(col, 2), ch)
    core = lax.rem(col, 2)
    mesh_id = pl.DeviceIdType.MESH

    barrier = pltpu.get_barrier_semaphore()
    targets = [at(*d) for d in around] + peers + [mate]
    for t in targets:
        pl.semaphore_signal(barrier, inc=1, device_id=t, device_id_type=mesh_id)

    def remote(src, dst, ssem, rsem, to):
        return pltpu.make_async_remote_copy(
            src_ref=src, dst_ref=dst, send_sem=ssem, recv_sem=rsem, device_id=to, device_id_type=mesh_id
        )

    part, pw, fw, gw = width // n, projw_h.shape[1], fc1w_h.shape[2], fc2w_h.shape[1]

    def slots(b, owner, halves):
        out = []
        for i, size in enumerate((part, pw, width, gw)):
            start = owner * size if i != 2 else 0
            if halves[i]:
                size = size // 2
                start = start + core * size
            span = pl.ds(pl.multiple_of(start, 16), size)
            lanes = pl.ds(pl.multiple_of(owner * fw, 128), fw)
            out.append((
                lambda: qkv.at[b, :, span, :], lambda: proj.at[b, span, :],
                lambda: fc1.at[b, span, lanes], lambda: fc2.at[b, span, :],
            )[i]())
        return out

    loads = {}
    for i, (name, s, d) in enumerate([
        ("table", table_h, table), ("qb", qkvb_h, qb_all.at[ch]), ("f1b", fc1b_h, f1b_all.at[ch]),
        ("qkv", qkvw_h, qkv.at[:, :, pl.ds(pl.multiple_of(ch * part, 16), part), :]),
        ("proj", projw_h, proj.at[:, pl.ds(pl.multiple_of(ch * pw, 16), pw), :]),
        ("fc1", fc1w_h, fc1.at[:, :, pl.ds(pl.multiple_of(ch * fw, 128), fw)]),
        ("fc2", fc2w_h, fc2.at[:, pl.ds(pl.multiple_of(ch * gw, 16), gw), :]),
        ("lab", lab_h, lab), ("x", x_h, x_v), ("gain", gain_h, gain), ("shift", shift_h, shift),
        ("rel", rel_h, rel), ("proj_b", projb_h, proj_b), ("fc2_b", fc2b_h, fc2_b),
    ]):
        loads[name] = pltpu.make_async_copy(s, d, in_sem.at[i])
        loads[name].start()
    tab_all[ch, :, :, :] = jnp.zeros(tab_all.shape[1:], f32)
    loads["table"].wait()
    tab_all[ch, :, : table.shape[1], : table.shape[2]] = table[...]
    pl.semaphore_wait(barrier, len(targets))

    split = {0: (False, True, True, True), 1: (True, True, True, True)}
    direct, relays, smalls = {}, {}, []
    for d in range(1, n):
        to, owner = peers[d - 1], lax.rem(ch - d + n, n)
        for b in range(BLOCKS):
            for i, s in enumerate(slots(b, ch, split[b])):
                direct[d, b, i] = remote(s, s, wsend.at[d - 1, b, i], wrecv.at[d - 1, b, i], to)
            for i, s in enumerate(slots(b, owner, split[b])):
                if split[b][i]:
                    relays[d, b, i] = remote(s, s, rsend.at[d - 1, b, i], rrecv.at[d - 1, b, i], mate)
        for i, ref in enumerate([tab_all, qb_all, f1b_all]):
            smalls.append(remote(ref.at[ch], ref.at[ch], ssend.at[d - 1, i], srecv.at[d - 1, i], to))
    loads["qkv"].wait()
    for d in range(1, n):
        direct[d, 0, 0].start()
    loads["qb"].wait()
    loads["f1b"].wait()
    for c in smalls:
        c.start()
    for name in ("proj", "fc1", "fc2", "lab"):
        loads[name].wait()
    labels = []
    for i, d in enumerate(around[:3]):
        labels.append(remote(lab, lab3.at[i], lsend.at[i], lrecv.at[i], at(*d)))
        labels[-1].start()
    for b in range(BLOCKS):
        for d in range(1, n):
            for i in range(b == 0, 4):
                direct[d, b, i].start()

    for name in ("x", "gain", "shift", "rel", "proj_b", "fc2_b"):
        loads[name].wait()

    def here(k, more=0):
        return pl.ds(k * group, group + more)

    def prepare(k, _):
        t = quads(x_v[:, pl.ds(pl.multiple_of(k * group * WIN, WIN), group * WIN), :].astype(f32))
        xq[here(k)] = t.astype(bf16).reshape(group, KEYS, width)
        nq[here(k)] = layer_norm(t, gain[0, 0:1], shift[0, 0:1]).reshape(group, KEYS, width)
        return 0

    lax.fori_loop(0, chunks, prepare, 0)

    idx = quads(jnp.concatenate([rel[...]] * 2, axis=1).reshape(WIN, WIN, 128))
    lane = lax.broadcasted_iota(i32, (KEYS, 128), 1)
    a, c = place_of(lane & (KEYS - 1))
    idx = jnp.take_along_axis(idx, (lane & KEYS) + a * WIN + c, axis=1, mode="promise_in_bounds")
    for c in smalls:
        c.wait_recv()
    scale = (width // heads) ** (-0.5) * LOG2E
    for j in range(n):
        for b in range(BLOCKS):
            for m in range(3):
                qb[b, :, m * width + j * part : m * width + (j + 1) * part] = qb_all[j, m, b : b + 1, :]
            f1b[b, :, j * fw : (j + 1) * fw] = f1b_all[j, b : b + 1, :]
    local_heads = table.shape[1]
    for b in range(BLOCKS):
        for t in range(heads // 2):
            out = []
            for h in (2 * t, 2 * t + 1):
                entry = tab_all[h // local_heads, b, h % local_heads : h % local_heads + 1, :]
                got = None
                for c in range(0, entry.shape[1], 128):
                    piece = jnp.broadcast_to(entry[:, c : c + 128], idx.shape)
                    piece = jnp.take_along_axis(piece, idx & 127, axis=1, mode="promise_in_bounds")
                    got = piece if got is None else jnp.where(idx >= c, piece, got)
                out.append(got)
            bias[b, :, t * 128 : (t + 1) * 128] = jnp.where(lane < KEYS, out[0], out[1]) * LOG2E

    hmask = head_mask(heads, KEYS, width)
    lanes3 = lax.broadcasted_iota(i32, (1, 3 * width), 1)
    mult = jnp.where(lanes3 < width, scale, 1.0)

    def project(normed, b):
        return ((dot_t(normed, rows_of(qkv[b])) + qb[b]) * mult).astype(bf16)

    def regions():
        for c in labels:
            c.wait_recv()
        kind = jnp.concatenate([lab[SHIFT:], lab3[0, :SHIFT]], axis=0).astype(f32)
        kind = pltpu.roll(kind, cols - SHIFT, 1)
        wrap = jnp.concatenate([lab3[1, SHIFT:, :128], lab3[2, :SHIFT, :128]], axis=0).astype(f32)
        wrap = jnp.concatenate([jnp.zeros((rows, cols - 128), f32), pltpu.roll(wrap, 128 - SHIFT, 1)], axis=1)
        i = lax.broadcasted_iota(i32, (rows, cols), 0)
        j = lax.broadcasted_iota(i32, (rows, cols), 1)
        def flag(where, when):
            return jnp.where(where, when.astype(f32), 0.0)
        kind = jnp.where(j >= cols - SHIFT, wrap, kind) * 4.0
        kind = kind + flag(i >= SHIFT, ring == total - 1) * 2.0 + flag(j >= cols - SHIFT, col == ncol - 1)
        lane8 = lax.broadcasted_iota(i32, (rows, 128), 1)
        per = 128 // WIN
        stack = []
        for c in range(WIN):
            got = None
            for p in range(0, cols, 128):
                piece = jnp.take_along_axis(
                    kind[:, p : p + 128], (lane8 & (per - 1)) * WIN + c, axis=1, mode="promise_in_bounds"
                )
                got = piece if got is None else jnp.where(lane8 >= p // WIN, piece, got)
            stack.append(got)
        stack = jnp.concatenate(stack, axis=0).astype(bf16)
        a, c = place_of(lax.broadcasted_iota(i32, (128, KEYS), 0) & (KEYS - 1))
        pick = (c * WIN + a == lax.broadcasted_iota(i32, (128, KEYS), 1)).astype(f32).astype(bf16)
        kinds = dot(pick, stack)
        ru[...] = kinds.T
        for j in range(nwin):
            rt[j] = jnp.broadcast_to(kinds[:KEYS, j : j + 1], (KEYS, 128))

    def mix(x, attended, b):
        middle = (x + dot(attended, proj[b]) + proj_b[b : b + 1]).astype(bf16).astype(f32)
        return middle, layer_norm(middle, gain[b, 1:2], shift[b, 1:2])

    def feed(middle, normed, b):
        inner = (dot(normed, fc1[b]) + f1b[b]).astype(bf16)
        hidden = inner * (lax.erf(inner * bf16(0.5 ** 0.5)) + bf16(1.0))
        outer = dot(hidden, fc2[b] * bf16(0.5))
        return (middle + outer + fc2_b[b : b + 1]).astype(bf16)

    def halo(k):
        return remote(x1.at[here(k), : 2 * PART, :], below.at[here(k)], hsend.at[k], hrecv.at[k], at(-1, 0))

    edges = [
        remote(x1.at[0, 2 * PART : 3 * PART], x1.at[nwin, 2 * PART : 3 * PART], esend.at[0], erecv.at[0], at(0, -1)),
        remote(x1.at[0, :PART], below.at[nwin, :PART], esend.at[1], erecv.at[1], at(-1, -1)),
    ]

    def back(k):
        return remote(
            yr.at[here(k)], yt.at[pl.ds(k * group + 1, group)], osend.at[k], orecv.at[k], at(1, 0)
        )

    fringe = [
        remote(yo.at[nwin, PART :], yo.at[0, PART :], fsend.at[0], frecv.at[0], at(0, 1)),
        remote(yr.at[nwin - 1, PART :], yt.at[0, PART :], fsend.at[1], frecv.at[1], at(1, 1)),
    ]

    def bring(b):
        for d in range(1, n):
            for i in range(4):
                direct[d, b, i].wait_recv()
                if (d, b, i) in relays:
                    relays[d, b, i].start()

    def settle(b):
        for d in range(1, n):
            for i in range(4):
                if (d, b, i) in relays:
                    relays[d, b, i].wait_recv()

    def block0(k):
        st = {}

        def score():
            st["triple"] = project(rows_of(nq[here(k)]), 0)
            st["scores"] = scores_of(st["triple"], hmask, heads)

        def soften():
            st["att"] = blend(weigh(st["scores"], bias[0], None), st["triple"], hmask, heads)

        def middle():
            if k == last:
                settle(0)
            st["mid"] = mix(rows_of(xq[here(k)]).astype(f32), jnp.concatenate(st["att"], axis=0), 0)

        def close():
            x1[here(k)] = feed(*st["mid"], 0).reshape(group, KEYS, width)
            halo(k).start()
            if k == 0:
                for c in edges:
                    c.start()

        return [score, soften, middle, close]

    def own_half(k):
        out = []
        for g in range(k * group, (k + 1) * group):
            out += [x1[g, 3 * PART :], x1[g + 1, 2 * PART : 3 * PART]]
        return out

    def far_half(k):
        out = []
        for g in range(k * group, (k + 1) * group):
            out += [below[g, PART :], below[g + 1, :PART]]
        return out

    def block1(k):
        st = {}

        def score():
            for h in {last - 1: (last, last - 1), last: ()}.get(k, (k,)):
                halo(h).wait_recv()
            if k == last:
                for c in edges:
                    c.wait_recv()
            mine, other = own_half(k), far_half(k)
            toks = []
            for g in range(group):
                toks += mine[2 * g : 2 * g + 2] + other[2 * g : 2 * g + 2]
            toks = jnp.concatenate(toks, axis=0).astype(f32)
            st["triple"] = project(layer_norm(toks, gain[1, 0:1], shift[1, 0:1]), 1)
            st["scores"] = scores_of(st["triple"], hmask, heads)

        def soften():
            masks = [rt[g] == ru[g : g + 1, :] for g in range(k * group, (k + 1) * group)]
            outs = blend(weigh(st["scores"], bias[1], masks), st["triple"], hmask, heads)
            st["att"] = [o[2 * PART :] for o in outs]
            for g, o in enumerate(outs):
                att[k * group + g] = o[: 2 * PART]

        def middle():
            x = jnp.concatenate(far_half(k), axis=0).astype(f32)
            st["mid"] = mix(x, jnp.concatenate(st["att"], axis=0), 1)

        def close():
            yr[here(k)] = feed(*st["mid"], 1).reshape(group, 2 * PART, width)
            back(k).start()
            if k == last:
                fringe[1].start()

        return [score, soften, middle, close]

    def own(ks):
        st = {}

        def middle():
            x = jnp.concatenate(sum([own_half(k) for k in ks], []), axis=0).astype(f32)
            y = jnp.concatenate([rows_of(att[here(k)]) for k in ks], axis=0)
            st["mid"] = mix(x, y, 1)

        def close():
            y = feed(*st["mid"], 1).reshape(len(ks), group, 2 * PART, width)
            for i, k in enumerate(ks):
                yo[pl.ds(k * group + 1, group)] = y[i]
            if last in ks:
                fringe[0].start()

        return [None, None, middle, close]

    last = chunks - 1
    bring(0)
    pipeline([block0(k) for k in range(last, -1, -1)], 4)
    bring(1)
    regions()
    settle(1)
    order = list(range(last - 1, -1, -1)) + [last]
    owns = [own(order[::-1][i : i + 2]) for i in range(0, chunks, 2)]
    pipeline([block1(k) for k in order] + owns, 4)

    def place(src, base):
        v = src[...].astype(f32)
        for i in range(2):
            left, right = v[:nwin, PART + i * WIN : PART + (i + 1) * WIN], v[1:, i * WIN : (i + 1) * WIN]
            for r, y in enumerate(swap_halves(left, right)):
                o_ref[base + 2 * i + r] = y.reshape(cols, width).astype(bf16)

    fringe[0].wait_recv()
    place(yo, SHIFT)
    for k in range(chunks):
        back(k).wait_recv()
    fringe[1].wait_recv()
    place(yt, 0)
    for c in labels + smalls + edges + fringe + list(direct.values()) + list(relays.values()):
        c.wait_send()
    for k in range(chunks):
        halo(k).wait_send()
        back(k).wait_send()


def on_device(*args):
    x = args[0]
    rows, cols, width = x.shape
    n = lax.axis_size("ch")
    heads = args[7].shape[2] * n
    args = list(args)
    args[5] = args[5].swapaxes(2, 3)
    args[6] = args[6].swapaxes(0, 1)
    args[7] = args[7].swapaxes(1, 2)
    hidden = args[10].shape[2] * n
    nwin = cols // WIN
    group = max(d for d in range(1, MOST + 1) if nwin % d == 0)
    chunks = nwin // group
    assert rows == WIN and heads % 2 == 0 and chunks > 1
    dma = pltpu.SemaphoreType.DMA
    vm = pltpu.VMEM
    entries = args[7].shape[2] + -args[7].shape[2] % 128
    scratch = [
        vm(x.shape, bf16), vm((rows, cols), i32), vm(args[2].shape, i32), vm(args[3].shape, f32),
        vm(args[4].shape, f32), vm(args[7].shape, f32), vm(args[9].shape, f32), vm(args[13].shape, f32),
        vm((BLOCKS, 3, width, width), bf16), vm((BLOCKS, width, width), bf16),
        vm((BLOCKS, width, hidden), bf16), vm((BLOCKS, hidden, width), bf16),
        vm((n, BLOCKS, 8, entries), f32), vm((n,) + args[6].shape, f32), vm((n,) + args[11].shape, f32),
        vm((BLOCKS, 1, 3 * width), f32), vm((BLOCKS, 1, hidden), f32), vm((BLOCKS, KEYS, heads * KEYS), f32),
        vm((3, rows, cols), i32), vm((nwin, KEYS, 128), f32), vm((128, 128), f32),
        vm((nwin, KEYS, width), bf16), vm((nwin, KEYS, width), bf16), vm((nwin, 2 * PART, width), bf16),
        vm((nwin + 1, KEYS, width), bf16), vm((nwin + 1, 2 * PART, width), bf16),
        vm((nwin, 2 * PART, width), bf16), vm((nwin + 1, 2 * PART, width), bf16),
        vm((nwin + 1, 2 * PART, width), bf16),
        dma((14,)), dma((n - 1, 3)), dma((n - 1, 3)), dma((n - 1, BLOCKS, 4)), dma((n - 1, BLOCKS, 4)),
        dma((n - 1, BLOCKS, 4)), dma((n - 1, BLOCKS, 4)), dma((3,)), dma((3,)),
        dma((chunks,)), dma((chunks,)), dma((2,)), dma((2,)),
        dma((chunks,)), dma((chunks,)), dma((2,)), dma((2,)),
    ]
    return pl.pallas_call(
        functools.partial(fused, heads, group),
        out_shape=vm(x.shape, bf16),
        in_specs=[pl.BlockSpec(memory_space=pl.ANY)] * len(args),
        out_specs=pl.BlockSpec(memory_space=vm),
        scratch_shapes=scratch,
        compiler_params=pltpu.CompilerParams(
            collective_id=0, has_side_effects=True, vmem_limit_bytes=56 * 1024 * 1024
        ),
        name="fused",
    )(*args)


def solution(mesh):
    in_specs = (
        P(("row", "ch"), "col", None), P(("row", "ch"), "col"), P(), P(), P(),
        P(None, None, None, "ch"), P(None, None, "ch"), P(None, None, "ch"), P(None, "ch", None), P(),
        P(None, None, "ch"), P(None, "ch"), P(None, "ch", None), P(),
    )
    out_specs = P(("row", "ch"), "col", None)
    return jax.shard_map(on_device, mesh=mesh, in_specs=in_specs, out_specs=out_specs, check_vma=False)
```

```python
import functools

import jax
import jax.numpy as jnp
from jax import lax
from jax.experimental import pallas as pl
from jax.experimental.pallas import tpu as pltpu
from jax.sharding import PartitionSpec as P

WIN = 8
SHIFT = 4
BLOCKS = 2
EPS = 1e-05
FAR = -1e30
LOG2E = 1.4426950408889634
MOST = 8
ORDER = ("middle", "score", "close", "soften")
bf16 = jnp.bfloat16
f32 = jnp.float32
i32 = jnp.int32
KEYS = WIN * WIN
PART = SHIFT * SHIFT


def dot(a, b):
    return jnp.dot(a, b, preferred_element_type=f32)


def dot_t(a, b):
    return lax.dot_general(a, b, (((1,), (1,)), ((), ())), preferred_element_type=f32)


def layer_norm(x, gain, offset):
    center = x - jnp.mean(x, axis=-1, keepdims=True)
    spread = jnp.mean(center * center, axis=-1, keepdims=True)
    return (center * lax.rsqrt(spread + EPS) * gain + offset).astype(bf16)


def rows_of(x):
    return x.reshape(x.shape[0] * x.shape[1], x.shape[2])


def swap_halves(e, o):
    low = lax.broadcasted_iota(i32, e.shape, 1) < SHIFT
    return jnp.where(low, e, pltpu.roll(o, SHIFT, 1)), jnp.where(low, pltpu.roll(e, SHIFT, 1), o)


def quads(x):
    rows, wide, width = x.shape
    g = wide // WIN
    pairs = []
    for r in range(0, rows, 2):
        pairs.append(swap_halves(x[r].reshape(g, WIN, width), x[r + 1].reshape(g, WIN, width)))
    parts = []
    for w in range(g):
        for h in range(0, rows // 2, 2):
            parts += [pairs[h + i][s][w] for s in (0, 1) for i in (0, 1)]
    return jnp.concatenate(parts, axis=0)


def place_of(t):
    q, i = t >> 4, t & 15
    return SHIFT * (q >> 1) + (i >> 2), SHIFT * (q & 1) + (i & 3)


def head_mask(heads, keys, width):
    depth = width // heads
    row = lax.broadcasted_iota(i32, (heads * keys, width), 0) // keys
    col = lax.broadcasted_iota(i32, (heads * keys, width), 1) // depth
    return (row == col).astype(f32).astype(bf16)


def scores_of(triple, hmask, heads, rows):
    width = triple.shape[1] // 3
    out = []
    for w in range(0, triple.shape[0], KEYS):
        q, k = triple[w : w + KEYS, :width][rows], triple[w : w + KEYS, width : 2 * width]
        out.append(dot_t(q, jnp.concatenate([k] * heads, axis=0) * hmask))
    return out


def weigh(scores, bias, masks):
    low = lax.broadcasted_iota(i32, (bias.shape[0], 128), 1) < KEYS
    weights = []
    for w, s in enumerate(scores):
        parts = []
        for c in range(0, s.shape[1], 128):
            t = s[:, c : c + 128] + bias[:, c : c + 128]
            if masks is not None:
                t = jnp.where(masks[w], t, FAR)
            u = t.astype(bf16)
            first = jnp.max(jnp.where(low, u, bf16(-jnp.inf)), axis=-1, keepdims=True)
            second = jnp.max(jnp.where(low, bf16(-jnp.inf), u), axis=-1, keepdims=True)
            parts.append(jnp.exp2(t - jnp.where(low, first, second).astype(f32)))
        weights.append(jnp.concatenate(parts, axis=1).astype(bf16))
    return weights


def blend(weights, triple, hmask, heads):
    width = triple.shape[1] // 3
    outs = []
    for w, p in enumerate(weights):
        v = triple[w * KEYS : (w + 1) * KEYS, 2 * width :]
        o = dot(p, jnp.concatenate([jnp.concatenate([v] * heads, axis=0) * hmask, hmask], axis=1))
        outs.append((o[:, :width] / o[:, width:]).astype(bf16))
    return outs


def overlap(now, before):
    if now is not None:
        now["wait"]()
    for stage in ORDER:
        task = now if stage in ("score", "soften") else before
        if task is not None:
            task[stage]()


def fused(
    heads, group,
    x_h, lab_h, rel_h, gain_h, shift_h, qkvw_h, qkvb_h, table_h, projw_h, projb_h, fc1w_h, fc1b_h, fc2w_h, fc2b_h,
    o_ref,
    x_v, lab, rel, gain, shift, proj_b, fc2_b,
    qkv, proj, fc1, fc2, tab_all, qb_all, f1b_all, qb, f1b, bias, lab3, rt, ru,
    xq, nq, tri, x1, below, yr, yt, yo,
    in_sem, ssend, srecv, wsend, wrecv, rsend, rrecv, lsend, lrecv, hsend, hrecv, esend, erecv,
    osend, orecv, fsend, frecv,
):
    rows, cols, width = x_v.shape
    nwin = cols // WIN
    chunks = nwin // group
    n = lax.axis_size("ch")
    nrow, ncol = lax.axis_size("row"), lax.axis_size("col")
    row, col, ch = lax.axis_index("row"), lax.axis_index("col"), lax.axis_index("ch")
    ring = row * n + ch
    total = nrow * n

    def at(dr, dc):
        p = lax.rem(ring + dr + total, total)
        return (p // n, lax.rem(col + dc + ncol, ncol), lax.rem(p, n))

    around = [(-1, 0), (0, -1), (-1, -1), (1, 0), (0, 1), (1, 1)]
    peers = [(row, col, lax.rem(ch + d, n)) for d in range(1, n)]
    mate = (row, col + 1 - 2 * lax.rem(col, 2), ch)
    core = lax.rem(col, 2)
    mesh_id = pl.DeviceIdType.MESH

    barrier = pltpu.get_barrier_semaphore()
    targets = [at(*d) for d in around] + peers + [mate]
    for t in targets:
        pl.semaphore_signal(barrier, inc=1, device_id=t, device_id_type=mesh_id)

    def remote(src, dst, ssem, rsem, to):
        return pltpu.make_async_remote_copy(
            src_ref=src, dst_ref=dst, send_sem=ssem, recv_sem=rsem, device_id=to, device_id_type=mesh_id
        )

    part, pw, fw, gw = width // n, projw_h.shape[1], fc1w_h.shape[2], fc2w_h.shape[1]

    def slots(b, owner, halves):
        out = []
        for i, size in enumerate((part, pw, width, gw)):
            start = owner * size if i != 2 else 0
            if halves[i]:
                size = size // 2
                start = start + core * size
            span = pl.ds(pl.multiple_of(start, 16), size)
            lanes = pl.ds(pl.multiple_of(owner * fw, 128), fw)
            out.append((
                lambda: qkv.at[b, :, span, :], lambda: proj.at[b, span, :],
                lambda: fc1.at[b, span, lanes], lambda: fc2.at[b, span, :],
            )[i]())
        return out

    loads = {}
    for i, (name, s, d) in enumerate([
        ("table", table_h, tab_all.at[ch]), ("qb", qkvb_h, qb_all.at[ch]), ("f1b", fc1b_h, f1b_all.at[ch]),
        ("qkv", qkvw_h, qkv.at[:, :, pl.ds(pl.multiple_of(ch * part, 16), part), :]),
        ("proj", projw_h, proj.at[:, pl.ds(pl.multiple_of(ch * pw, 16), pw), :]),
        ("fc1", fc1w_h, fc1.at[:, :, pl.ds(pl.multiple_of(ch * fw, 128), fw)]),
        ("fc2", fc2w_h, fc2.at[:, pl.ds(pl.multiple_of(ch * gw, 16), gw), :]),
        ("lab", lab_h, lab), ("x", x_h, x_v), ("gain", gain_h, gain), ("shift", shift_h, shift),
        ("rel", rel_h, rel), ("proj_b", projb_h, proj_b), ("fc2_b", fc2b_h, fc2_b),
    ]):
        loads[name] = pltpu.make_async_copy(s, d, in_sem.at[i])
        loads[name].start()
    pl.semaphore_wait(barrier, len(targets))

    split = {0: (False, False, True, True), 1: (True, True, True, True)}
    direct, relays, smalls = {}, {}, []
    for d in range(1, n):
        to, owner = peers[d - 1], lax.rem(ch - d + n, n)
        for b in range(BLOCKS):
            for i, s in enumerate(slots(b, ch, split[b])):
                direct[d, b, i] = remote(s, s, wsend.at[d - 1, b, i], wrecv.at[d - 1, b, i], to)
            for i, s in enumerate(slots(b, owner, split[b])):
                if split[b][i]:
                    relays[d, b, i] = remote(s, s, rsend.at[d - 1, b, i], rrecv.at[d - 1, b, i], mate)
        for i, ref in enumerate([tab_all, qb_all, f1b_all]):
            smalls.append(remote(ref.at[ch], ref.at[ch], ssend.at[d - 1, i], srecv.at[d - 1, i], to))
    loads["lab"].wait()
    labels = []
    for i, d in enumerate(around[:3]):
        labels.append(remote(lab, lab3.at[i], lsend.at[i], lrecv.at[i], at(*d)))
        labels[-1].start()
    for name in ("table", "qb", "f1b", "qkv", "proj", "fc1", "fc2"):
        loads[name].wait()
    for c in smalls:
        c.start()
    for b in range(BLOCKS):
        for i in range(4):
            for d in range(1, n):
                direct[d, b, i].start()
    for name in ("x", "gain", "shift", "rel", "proj_b", "fc2_b"):
        loads[name].wait()

    def here(k, more=0):
        return pl.ds(k * group, group + more)

    def prepare(k, _):
        t = quads(x_v[:, pl.ds(pl.multiple_of(k * group * WIN, WIN), group * WIN), :].astype(f32))
        xq[here(k)] = t.astype(bf16).reshape(group, KEYS, width)
        nq[here(k)] = layer_norm(t, gain[0, 0:1], shift[0, 0:1]).reshape(group, KEYS, width)
        return 0

    lax.fori_loop(0, chunks, prepare, 0)

    idx = quads(jnp.concatenate([rel[...]] * 2, axis=1).reshape(WIN, WIN, 128))
    lane = lax.broadcasted_iota(i32, (KEYS, 128), 1)
    a, c = place_of(lane & (KEYS - 1))
    idx = jnp.take_along_axis(idx, (lane & KEYS) + a * WIN + c, axis=1, mode="promise_in_bounds")
    for c in smalls:
        c.wait_recv()
    scale = (width // heads) ** (-0.5) * LOG2E
    for j in range(n):
        for b in range(BLOCKS):
            for m in range(3):
                qb[b, :, m * width + j * part : m * width + (j + 1) * part] = qb_all[j, m, b : b + 1, :]
            f1b[b, :, j * fw : (j + 1) * fw] = f1b_all[j, b : b + 1, :]
    local_heads, entries = table_h.shape[1:]
    for b in range(BLOCKS):
        for t in range(heads // 2):
            out = []
            for h in (2 * t, 2 * t + 1):
                entry = tab_all[h // local_heads, b, h % local_heads : h % local_heads + 1, :]
                got = None
                for c in range(0, entries, 128):
                    piece = entry[:, c : c + 128]
                    if piece.shape[1] < 128:
                        piece = jnp.concatenate([piece, jnp.zeros((1, 128 - piece.shape[1]), f32)], axis=1)
                    piece = jnp.broadcast_to(piece, idx.shape)
                    piece = jnp.take_along_axis(piece, idx & 127, axis=1, mode="promise_in_bounds")
                    got = piece if got is None else jnp.where(idx >= c, piece, got)
                out.append(got)
            bias[b, :, t * 128 : (t + 1) * 128] = jnp.where(lane < KEYS, out[0], out[1]) * LOG2E

    hmask = head_mask(heads, KEYS, width)
    lanes3 = lax.broadcasted_iota(i32, (1, 3 * width), 1)
    mult = jnp.where(lanes3 < width, scale, 1.0)

    def project(normed, b):
        return ((dot_t(normed, rows_of(qkv[b])) + qb[b]) * mult).astype(bf16)

    def regions():
        for c in labels:
            c.wait_recv()
        kind = jnp.concatenate([lab[SHIFT:], lab3[0, :SHIFT]], axis=0).astype(f32)
        kind = pltpu.roll(kind, cols - SHIFT, 1)
        wrap = jnp.concatenate([lab3[1, SHIFT:, :128], lab3[2, :SHIFT, :128]], axis=0).astype(f32)
        wrap = jnp.concatenate([jnp.zeros((rows, cols - 128), f32), pltpu.roll(wrap, 128 - SHIFT, 1)], axis=1)
        i = lax.broadcasted_iota(i32, (rows, cols), 0)
        j = lax.broadcasted_iota(i32, (rows, cols), 1)
        def flag(where, when):
            return jnp.where(where, when.astype(f32), 0.0)
        kind = jnp.where(j >= cols - SHIFT, wrap, kind) * 4.0
        kind = kind + flag(i >= SHIFT, ring == total - 1) * 2.0 + flag(j >= cols - SHIFT, col == ncol - 1)
        lane8 = lax.broadcasted_iota(i32, (rows, 128), 1)
        per = 128 // WIN
        stack = []
        for c in range(WIN):
            got = None
            for p in range(0, cols, 128):
                piece = jnp.take_along_axis(
                    kind[:, p : p + 128], (lane8 & (per - 1)) * WIN + c, axis=1, mode="promise_in_bounds"
                )
                got = piece if got is None else jnp.where(lane8 >= p // WIN, piece, got)
            stack.append(got)
        stack = jnp.concatenate(stack, axis=0).astype(bf16)
        a, c = place_of(lax.broadcasted_iota(i32, (128, KEYS), 0) & (KEYS - 1))
        pick = (c * WIN + a == lax.broadcasted_iota(i32, (128, KEYS), 1)).astype(f32).astype(bf16)
        kinds = dot(pick, stack)
        ru[...] = kinds.T
        rt[...] = kinds[:KEYS]

    def mix(x, attended, b):
        middle = (x + dot(attended, proj[b]) + proj_b[b : b + 1]).astype(bf16).astype(f32)
        return middle, layer_norm(middle, gain[b, 1:2], shift[b, 1:2])

    def feed(middle, normed, b):
        inner = (dot(normed, fc1[b]) + f1b[b]).astype(bf16)
        hidden = inner * (lax.erf(inner * bf16(0.5 ** 0.5)) + bf16(1.0))
        outer = dot(hidden, fc2[b] * bf16(0.5))
        return (middle + outer + fc2_b[b : b + 1]).astype(bf16)

    def halo(k):
        return remote(x1.at[here(k), : 2 * PART, :], below.at[here(k)], hsend.at[k], hrecv.at[k], at(-1, 0))

    edges = [
        remote(x1.at[0, 2 * PART : 3 * PART], x1.at[nwin, 2 * PART : 3 * PART], esend.at[0], erecv.at[0], at(0, -1)),
        remote(x1.at[0, :PART], below.at[nwin, :PART], esend.at[1], erecv.at[1], at(-1, -1)),
    ]

    spans = [(k * group, group - (k == chunks - 1)) for k in range(chunks)] + [(nwin - 1, 1)]

    def back(i):
        start, size = spans[i]
        return remote(
            yr.at[pl.ds(start, size)], yt.at[pl.ds(start + 1, size)], osend.at[i], orecv.at[i], at(1, 0)
        )

    fringe = [
        remote(yo.at[nwin, PART :], yo.at[0, PART :], fsend.at[0], frecv.at[0], at(0, 1)),
        remote(yr.at[nwin - 1, PART :], yt.at[0, PART :], fsend.at[1], frecv.at[1], at(1, 1)),
    ]

    def bring(b, pieces):
        for i in pieces:
            for d in range(1, n):
                direct[d, b, i].wait_recv()
                if (d, b, i) in relays:
                    relays[d, b, i].start()

    def settle(b):
        for d in range(1, n):
            for i in range(4):
                if (d, b, i) in relays:
                    relays[d, b, i].wait_recv()

    def block0(k):
        st = {}

        def wait():
            pass

        def score():
            st["triple"] = project(rows_of(nq[here(k)]), 0)
            st["scores"] = scores_of(st["triple"], hmask, heads, slice(None))

        def soften():
            st["att"] = blend(weigh(st["scores"], bias[0], None), st["triple"], hmask, heads)

        def middle():
            st["mid"] = mix(rows_of(xq[here(k)]).astype(f32), jnp.concatenate(st["att"], axis=0), 0)

        def close():
            x1[here(k)] = feed(*st["mid"], 0).reshape(group, KEYS, width)
            halo(k).start()
            if k == 0:
                for c in edges:
                    c.start()

        return {"wait": wait, "score": score, "soften": soften, "middle": middle, "close": close}

    def own_half(ws):
        return sum([[x1[w, 3 * PART :], x1[w + 1, 2 * PART : 3 * PART]] for w in ws], [])

    def far_half(ws):
        return sum([[below[w, PART :], below[w + 1, :PART]] for w in ws], [])

    near, far = slice(0, 2 * PART), slice(2 * PART, KEYS)

    def masks(ws, part):
        return [jnp.broadcast_to(rt[part, w : w + 1], (2 * PART, 128)) == ru[w : w + 1, :] for w in ws]

    def split_rows(x):
        return [x[i : i + 2 * PART] for i in range(0, x.shape[0], 2 * PART)]

    def block1(ids, halos):
        st = {}
        ws = [w for i in ids for w in range(spans[i][0], sum(spans[i]))]

        def wait():
            for c in halos:
                c.wait_recv()

        def score():
            mine, other = own_half(ws), far_half(ws)
            toks = []
            for g in range(0, 2 * len(ws), 2):
                toks += mine[g : g + 2] + other[g : g + 2]
            toks = jnp.concatenate(toks, axis=0).astype(f32)
            st["triple"] = project(layer_norm(toks, gain[1, 0:1], shift[1, 0:1]), 1)
            for i, w in enumerate(ws):
                tri[w] = st["triple"][i * KEYS : (i + 1) * KEYS]
            st["scores"] = scores_of(st["triple"], hmask, heads, far)

        def soften():
            st["att"] = blend(weigh(st["scores"], bias[1, far, :], masks(ws, far)), st["triple"], hmask, heads)

        def middle():
            x = jnp.concatenate(far_half(ws), axis=0).astype(f32)
            st["mid"] = mix(x, jnp.concatenate(st["att"], axis=0), 1)

        def close():
            for w, y in zip(ws, split_rows(feed(*st["mid"], 1))):
                yr[w] = y
            for i in ids:
                back(i).start()
            if nwin - 1 in ws:
                fringe[1].start()

        return {"wait": wait, "score": score, "soften": soften, "middle": middle, "close": close}

    def own(ws):
        st = {}

        def wait():
            pass

        def score():
            st["triple"] = jnp.concatenate([tri[w] for w in ws], axis=0)
            st["scores"] = scores_of(st["triple"], hmask, heads, near)

        def soften():
            st["att"] = blend(weigh(st["scores"], bias[1, near, :], masks(ws, near)), st["triple"], hmask, heads)

        def middle():
            x = jnp.concatenate(own_half(ws), axis=0).astype(f32)
            st["mid"] = mix(x, jnp.concatenate(st["att"], axis=0), 1)

        def close():
            for w, y in zip(ws, split_rows(feed(*st["mid"], 1))):
                yo[w + 1] = y
            if nwin - 1 in ws:
                fringe[0].start()

        return {"wait": wait, "score": score, "soften": soften, "middle": middle, "close": close}

    last = chunks - 1
    first = [block0(k) for k in range(last, -1, -1)]
    bring(0, (0,))
    overlap(first[0], None)
    bring(0, (1, 2, 3))
    regions()
    first[0]["middle"]()
    settle(0)
    first[0]["close"]()
    first[1]["score"]()
    first[1]["soften"]()
    bring(1, range(4))
    for t in range(1, chunks):
        overlap(first[t + 1] if t < last else None, first[t])
    settle(1)
    second = [block1([k], [halo(k)]) for k in range(last, 0, -1)] + [block1([0, chunks], [halo(0)] + edges)]
    half = nwin // 2
    second += [own([nwin - 1] + list(range(half - 1))), own(list(range(half - 1, nwin - 1)))]
    for t in range(len(second) + 1):
        overlap(second[t] if t < len(second) else None, second[t - 1] if t > 0 else None)

    def place(src, base):
        v = src[...].astype(f32)
        for i in range(2):
            left, right = v[:nwin, PART + i * WIN : PART + (i + 1) * WIN], v[1:, i * WIN : (i + 1) * WIN]
            for r, y in enumerate(swap_halves(left, right)):
                o_ref[base + 2 * i + r] = y.reshape(cols, width).astype(bf16)

    fringe[0].wait_recv()
    place(yo, SHIFT)
    for k in range(chunks + 1):
        back(k).wait_recv()
    fringe[1].wait_recv()
    place(yt, 0)
    for c in labels + smalls + edges + fringe + list(direct.values()) + list(relays.values()):
        c.wait_send()
    for k in range(chunks):
        halo(k).wait_send()
    for k in range(chunks + 1):
        back(k).wait_send()


def on_device(*args):
    x = args[0]
    rows, cols, width = x.shape
    n = lax.axis_size("ch")
    heads = args[7].shape[2] * n
    args = list(args)
    args[5] = args[5].swapaxes(2, 3)
    args[6] = args[6].swapaxes(0, 1)
    args[7] = args[7].swapaxes(1, 2)
    hidden = args[10].shape[2] * n
    nwin = cols // WIN
    group = max(d for d in range(1, MOST + 1) if nwin % d == 0)
    chunks = nwin // group
    assert rows == WIN and heads % 2 == 0 and chunks > 1
    dma = pltpu.SemaphoreType.DMA
    vm = pltpu.VMEM
    scratch = [
        vm(x.shape, bf16), vm((rows, cols), i32), vm(args[2].shape, i32), vm(args[3].shape, f32),
        vm(args[4].shape, f32), vm(args[9].shape, f32), vm(args[13].shape, f32),
        vm((BLOCKS, 3, width, width), bf16), vm((BLOCKS, width, width), bf16),
        vm((BLOCKS, width, hidden), bf16), vm((BLOCKS, hidden, width), bf16),
        vm((n,) + args[7].shape, f32), vm((n,) + args[6].shape, f32), vm((n,) + args[11].shape, f32),
        vm((BLOCKS, 1, 3 * width), f32), vm((BLOCKS, 1, hidden), f32), vm((BLOCKS, KEYS, heads * KEYS), f32),
        vm((3, rows, cols), i32), vm((KEYS, 128), f32), vm((128, 128), f32),
        vm((nwin, KEYS, width), bf16), vm((nwin, KEYS, width), bf16), vm((nwin, KEYS, 3 * width), bf16),
        vm((nwin + 1, KEYS, width), bf16), vm((nwin + 1, 2 * PART, width), bf16),
        vm((nwin, 2 * PART, width), bf16), vm((nwin + 1, 2 * PART, width), bf16),
        vm((nwin + 1, 2 * PART, width), bf16),
        dma((14,)), dma((n - 1, 3)), dma((n - 1, 3)), dma((n - 1, BLOCKS, 4)), dma((n - 1, BLOCKS, 4)),
        dma((n - 1, BLOCKS, 4)), dma((n - 1, BLOCKS, 4)), dma((3,)), dma((3,)),
        dma((chunks,)), dma((chunks,)), dma((2,)), dma((2,)),
        dma((chunks + 1,)), dma((chunks + 1,)), dma((2,)), dma((2,)),
    ]
    return pl.pallas_call(
        functools.partial(fused, heads, group),
        out_shape=vm(x.shape, bf16),
        in_specs=[pl.BlockSpec(memory_space=pl.ANY)] * len(args),
        out_specs=pl.BlockSpec(memory_space=vm),
        scratch_shapes=scratch,
        compiler_params=pltpu.CompilerParams(
            collective_id=0, has_side_effects=True, vmem_limit_bytes=56 * 1024 * 1024
        ),
        name="fused",
    )(*args)


def solution(mesh):
    in_specs = (
        P(("row", "ch"), "col", None), P(("row", "ch"), "col"), P(), P(), P(),
        P(None, None, None, "ch"), P(None, None, "ch"), P(None, None, "ch"), P(None, "ch", None), P(),
        P(None, None, "ch"), P(None, "ch"), P(None, "ch", None), P(),
    )
    out_specs = P(("row", "ch"), "col", None)
    return jax.shard_map(on_device, mesh=mesh, in_specs=in_specs, out_specs=out_specs, check_vma=False)
```

```python
import functools

import jax
import jax.numpy as jnp
from jax import lax
from jax.experimental import pallas as pl
from jax.experimental.pallas import tpu as pltpu
from jax.sharding import PartitionSpec as P

WIN = 8
SHIFT = 4
BLOCKS = 2
EPS = 1e-05
FAR = -1e30
LOG2E = 1.4426950408889634
MOST = 8
WHOLE = ((0, 1),)
ORDER = ("middle", "score", "close", "soften")
bf16 = jnp.bfloat16
f32 = jnp.float32
i32 = jnp.int32
KEYS = WIN * WIN
PART = SHIFT * SHIFT


def dot(a, b):
    return jnp.dot(a, b, preferred_element_type=f32)


def dot_t(a, b):
    return lax.dot_general(a, b, (((1,), (1,)), ((), ())), preferred_element_type=f32)


def layer_norm(x, gain, offset):
    center = x - jnp.mean(x, axis=-1, keepdims=True)
    spread = jnp.mean(center * center, axis=-1, keepdims=True)
    return (center * lax.rsqrt(spread + EPS) * gain + offset).astype(bf16)


def rows_of(x):
    return x.reshape(x.shape[0] * x.shape[1], x.shape[2])


def swap_halves(e, o):
    low = lax.broadcasted_iota(i32, e.shape, 1) < SHIFT
    return jnp.where(low, e, pltpu.roll(o, SHIFT, 1)), jnp.where(low, pltpu.roll(e, SHIFT, 1), o)


def quads(x):
    rows, wide, width = x.shape
    g = wide // WIN
    pairs = []
    for r in range(0, rows, 2):
        pairs.append(swap_halves(x[r].reshape(g, WIN, width), x[r + 1].reshape(g, WIN, width)))
    parts = []
    for w in range(g):
        for h in range(0, rows // 2, 2):
            parts += [pairs[h + i][s][w] for s in (0, 1) for i in (0, 1)]
    return jnp.concatenate(parts, axis=0)


def place_of(t):
    q, i = t >> 4, t & 15
    return SHIFT * (q >> 1) + (i >> 2), SHIFT * (q & 1) + (i & 3)


def head_mask(heads, keys, width):
    depth = width // heads
    row = lax.broadcasted_iota(i32, (heads * keys, width), 0) // keys
    col = lax.broadcasted_iota(i32, (heads * keys, width), 1) // depth
    return (row == col).astype(f32).astype(bf16)


def scores_of(triple, hmask, heads):
    width = triple.shape[1] // 3
    out = []
    for w in range(0, triple.shape[0], KEYS):
        q, k = triple[w : w + KEYS, :width], triple[w : w + KEYS, width : 2 * width]
        out.append(dot_t(q, jnp.concatenate([k] * heads, axis=0) * hmask))
    return out


def weigh(scores, bias, masks):
    low = lax.broadcasted_iota(i32, (bias.shape[0], 128), 1) < KEYS
    weights = []
    for w, s in enumerate(scores):
        parts = []
        for c in range(0, s.shape[1], 128):
            t = s[:, c : c + 128] + bias[:, c : c + 128]
            if masks is not None:
                t = jnp.where(masks[w], t, FAR)
            u = t.astype(bf16)
            first = jnp.max(jnp.where(low, u, bf16(-jnp.inf)), axis=-1, keepdims=True)
            second = jnp.max(jnp.where(low, bf16(-jnp.inf), u), axis=-1, keepdims=True)
            parts.append(jnp.exp2(t - jnp.where(low, first, second).astype(f32)))
        weights.append(jnp.concatenate(parts, axis=1).astype(bf16))
    return weights


def blend(weights, triple, hmask, heads):
    width = triple.shape[1] // 3
    outs = []
    for w, p in enumerate(weights):
        v = triple[w * KEYS : (w + 1) * KEYS, 2 * width :]
        o = dot(p, jnp.concatenate([jnp.concatenate([v] * heads, axis=0) * hmask, hmask], axis=1))
        outs.append((o[:, :width] / o[:, width:]).astype(bf16))
    return outs


def overlap(now, before):
    if now is not None:
        now["wait"]()
    for stage in ORDER:
        task = now if stage in ("score", "soften") else before
        if task is not None:
            task[stage]()


def fused(
    heads, group,
    x_h, lab_h, rel_h, gain_h, shift_h, qkvw_h, qkvb_h, table_h, projw_h, projb_h, fc1w_h, fc1b_h, fc2w_h, fc2b_h,
    o_ref,
    x_v, lab, rel, gain, shift, proj_b, fc2_b,
    qkv, proj, fc1, fc2, tab_all, qb_all, f1b_all, qb, f1b, bias, lab3, rt, ru,
    xq, nq, att, x1, above, yr, yt, yo,
    in_sem, ssend, srecv, wsend, wrecv, rsend, rrecv, lsend, lrecv, hsend, hrecv, esend, erecv,
    osend, orecv, fsend, frecv, ready,
):
    rows, cols, width = x_v.shape
    nwin = cols // WIN
    chunks = nwin // group
    n = lax.axis_size("ch")
    nrow, ncol = lax.axis_size("row"), lax.axis_size("col")
    row, col, ch = lax.axis_index("row"), lax.axis_index("col"), lax.axis_index("ch")
    ring = row * n + ch
    total = nrow * n

    def at(dr, dc):
        p = lax.rem(ring + dr + total, total)
        return (p // n, lax.rem(col + dc + ncol, ncol), lax.rem(p, n))

    around = [(1, 0), (0, -1), (1, -1), (-1, 0), (0, 1), (-1, 1)]
    peers = [(row, col, lax.rem(ch + d, n)) for d in range(1, n)]
    mate = (row, col + 1 - 2 * lax.rem(col, 2), ch)
    core = lax.rem(col, 2)
    mesh_id = pl.DeviceIdType.MESH

    barrier = pltpu.get_barrier_semaphore()
    targets = [at(*d) for d in around[3:]] + peers + [mate]
    for t in targets:
        pl.semaphore_signal(barrier, inc=1, device_id=t, device_id_type=mesh_id)

    def remote(src, dst, ssem, rsem, to):
        return pltpu.make_async_remote_copy(
            src_ref=src, dst_ref=dst, send_sem=ssem, recv_sem=rsem, device_id=to, device_id_type=mesh_id
        )

    part, pw, fw, gw = width // n, projw_h.shape[1], fc1w_h.shape[2], fc2w_h.shape[1]

    def slots(b, owner, share, count):
        out = []
        for i, size in enumerate((part, pw, width, gw)):
            start = owner * size if i != 2 else 0
            if (b, i) not in WHOLE:
                size = size // count
                start = start + share * size
            span = pl.ds(pl.multiple_of(start, 16), size)
            lanes = pl.ds(pl.multiple_of(owner * fw, 128), fw)
            out.append((
                lambda: qkv.at[b, :, span, :], lambda: proj.at[b, span, :],
                lambda: fc1.at[b, span, lanes], lambda: fc2.at[b, span, :],
            )[i]())
        return out

    loads = {}
    for i, (name, s, d) in enumerate([
        ("table", table_h, tab_all.at[ch]), ("qb", qkvb_h, qb_all.at[ch]), ("f1b", fc1b_h, f1b_all.at[ch]),
        ("qkv", qkvw_h, qkv.at[:, :, pl.ds(pl.multiple_of(ch * part, 16), part), :]),
        ("proj", projw_h, proj.at[:, pl.ds(pl.multiple_of(ch * pw, 16), pw), :]),
        ("fc1", fc1w_h, fc1.at[:, :, pl.ds(pl.multiple_of(ch * fw, 128), fw)]),
        ("fc2", fc2w_h, fc2.at[:, pl.ds(pl.multiple_of(ch * gw, 16), gw), :]),
        ("lab", lab_h, lab), ("x", x_h, x_v), ("gain", gain_h, gain), ("shift", shift_h, shift),
        ("rel", rel_h, rel), ("proj_b", projb_h, proj_b), ("fc2_b", fc2b_h, fc2_b),
    ]):
        loads[name] = pltpu.make_async_copy(s, d, in_sem.at[i])
        loads[name].start()
    pl.semaphore_wait(barrier, len(targets))
    for d in (around[0], around[2]):
        pl.semaphore_signal(ready, inc=1, device_id=at(*d), device_id_type=mesh_id)

    shares = {b: (core, 2, [mate]) for b in range(BLOCKS)}
    direct, relays, smalls = {}, {}, []
    for d in range(1, n):
        to, owner = peers[d - 1], lax.rem(ch - d + n, n)
        for b in range(BLOCKS):
            share, count, others = shares[b]
            for i, s in enumerate(slots(b, ch, share, count)):
                direct[d, b, i] = remote(s, s, wsend.at[d - 1, b, i], wrecv.at[d - 1, b, i], to)
            for e, other in enumerate(others):
                for i, s in enumerate(slots(b, owner, share, count)):
                    if (b, i) not in WHOLE:
                        r = b + e
                        relays[d, b, i, e] = remote(s, s, rsend.at[d - 1, r, i], rrecv.at[d - 1, r, i], other)
        for i, ref in enumerate([tab_all, qb_all, f1b_all]):
            smalls.append(remote(ref.at[ch], ref.at[ch], ssend.at[d - 1, i], srecv.at[d - 1, i], to))
    loads["lab"].wait()
    labels = []
    for i, d in enumerate(around[:3]):
        labels.append(remote(lab, lab3.at[i], lsend.at[i], lrecv.at[i], at(*d)))
        labels[-1].start()
    for name in ("table", "qb", "f1b", "qkv", "proj", "fc1", "fc2"):
        loads[name].wait()
    for c in smalls:
        c.start()
    for b in range(BLOCKS):
        for i in range(4):
            for d in range(1, n):
                direct[d, b, i].start()
    for name in ("x", "gain", "shift", "rel", "proj_b", "fc2_b"):
        loads[name].wait()

    def here(k, more=0):
        return pl.ds(k * group, group + more)

    def prepare(k, _):
        t = quads(x_v[:, pl.ds(pl.multiple_of(k * group * WIN, WIN), group * WIN), :].astype(f32))
        xq[here(k)] = t.astype(bf16).reshape(group, KEYS, width)
        nq[here(k)] = layer_norm(t, gain[0, 0:1], shift[0, 0:1]).reshape(group, KEYS, width)
        return 0

    lax.fori_loop(0, chunks, prepare, 0)

    idx = quads(jnp.concatenate([rel[...]] * 2, axis=1).reshape(WIN, WIN, 128))
    lane = lax.broadcasted_iota(i32, (KEYS, 128), 1)
    a, c = place_of(lane & (KEYS - 1))
    idx = jnp.take_along_axis(idx, (lane & KEYS) + a * WIN + c, axis=1, mode="promise_in_bounds")
    for c in smalls:
        c.wait_recv()
    scale = (width // heads) ** (-0.5) * LOG2E
    for j in range(n):
        for b in range(BLOCKS):
            for m in range(3):
                qb[b, :, m * width + j * part : m * width + (j + 1) * part] = qb_all[j, m, b : b + 1, :]
            f1b[b, :, j * fw : (j + 1) * fw] = f1b_all[j, b : b + 1, :]
    local_heads, entries = table_h.shape[1:]
    for b in range(BLOCKS):
        for t in range(heads // 2):
            out = []
            for h in (2 * t, 2 * t + 1):
                entry = tab_all[h // local_heads, b, h % local_heads : h % local_heads + 1, :]
                got = None
                for c in range(0, entries, 128):
                    piece = entry[:, c : c + 128]
                    if piece.shape[1] < 128:
                        piece = jnp.concatenate([piece, jnp.zeros((1, 128 - piece.shape[1]), f32)], axis=1)
                    piece = jnp.broadcast_to(piece, idx.shape)
                    piece = jnp.take_along_axis(piece, idx & 127, axis=1, mode="promise_in_bounds")
                    got = piece if got is None else jnp.where(idx >= c, piece, got)
                out.append(got)
            bias[b, :, t * 128 : (t + 1) * 128] = jnp.where(lane < KEYS, out[0], out[1]) * LOG2E

    hmask = head_mask(heads, KEYS, width)
    lanes3 = lax.broadcasted_iota(i32, (1, 3 * width), 1)
    mult = jnp.where(lanes3 < width, scale, 1.0)

    def project(normed, b):
        return ((dot_t(normed, rows_of(qkv[b])) + qb[b]) * mult).astype(bf16)

    def regions():
        for c in labels:
            c.wait_recv()
        kind = jnp.concatenate([lab3[0, SHIFT:], lab[:SHIFT]], axis=0).astype(f32)
        kind = pltpu.roll(kind, cols - SHIFT, 1)
        wrap = jnp.concatenate([lab3[2, SHIFT:, :128], lab3[1, :SHIFT, :128]], axis=0).astype(f32)
        wrap = jnp.concatenate([jnp.zeros((rows, cols - 128), f32), pltpu.roll(wrap, 128 - SHIFT, 1)], axis=1)
        i = lax.broadcasted_iota(i32, (rows, cols), 0)
        j = lax.broadcasted_iota(i32, (rows, cols), 1)
        def flag(where, when):
            return jnp.where(where, when.astype(f32), 0.0)
        kind = jnp.where(j >= cols - SHIFT, wrap, kind) * 4.0
        kind = kind + flag(i >= SHIFT, ring == 0) * 2.0 + flag(j >= cols - SHIFT, col == ncol - 1)
        lane8 = lax.broadcasted_iota(i32, (rows, 128), 1)
        per = 128 // WIN
        stack = []
        for c in range(WIN):
            got = None
            for p in range(0, cols, 128):
                piece = jnp.take_along_axis(
                    kind[:, p : p + 128], (lane8 & (per - 1)) * WIN + c, axis=1, mode="promise_in_bounds"
                )
                got = piece if got is None else jnp.where(lane8 >= p // WIN, piece, got)
            stack.append(got)
        stack = jnp.concatenate(stack, axis=0).astype(bf16)
        a, c = place_of(lax.broadcasted_iota(i32, (128, KEYS), 0) & (KEYS - 1))
        pick = (c * WIN + a == lax.broadcasted_iota(i32, (128, KEYS), 1)).astype(f32).astype(bf16)
        kinds = dot(pick, stack)
        ru[...] = kinds.T
        rt[...] = kinds[:KEYS]

    def mix(x, attended, b):
        middle = (x + dot(attended, proj[b]) + proj_b[b : b + 1]).astype(bf16).astype(f32)
        return middle, layer_norm(middle, gain[b, 1:2], shift[b, 1:2])

    def feed(middle, normed, b):
        inner = (dot(normed, fc1[b]) + f1b[b]).astype(bf16)
        hidden = inner * (lax.erf(inner * bf16(0.5 ** 0.5)) + bf16(1.0))
        outer = dot(hidden, fc2[b] * bf16(0.5))
        return (middle + outer + fc2_b[b : b + 1]).astype(bf16)

    cut = group // 2
    final = nwin - group
    heads_of = [(0, 1), (final, cut), (final + cut, group - cut)]
    heads_of += [(k * group, group) for k in range(chunks - 2, 0, -1)] + [(1, group - 1)]

    def halo(i):
        start, size = heads_of[i]
        span = pl.ds(start, size)
        return remote(x1.at[span, 2 * PART :, :], above.at[span], hsend.at[i], hrecv.at[i], at(1, 0))

    edges = [
        remote(x1.at[0, :PART], x1.at[nwin, :PART], esend.at[0], erecv.at[0], at(0, -1)),
        remote(x1.at[0, 2 * PART : 3 * PART], above.at[nwin, :PART], esend.at[1], erecv.at[1], at(1, -1)),
    ]

    spans = [(k * group, group) for k in range(chunks - 1, 0, -1)] + [(0, cut), (cut, group - cut)]

    def back(i):
        start, size = spans[i]
        return remote(
            yr.at[pl.ds(start, size)], yt.at[pl.ds(start + 1, size)], osend.at[i], orecv.at[i], at(-1, 0)
        )

    fringe = [
        remote(yo.at[nwin, PART :], yo.at[0, PART :], fsend.at[0], frecv.at[0], at(0, 1)),
        remote(yr.at[nwin - 1, PART :], yt.at[0, PART :], fsend.at[1], frecv.at[1], at(-1, 1)),
    ]

    def bring(b, pieces):
        for i in pieces:
            for d in range(1, n):
                direct[d, b, i].wait_recv()
                for e in range(len(shares[b][2])):
                    if (d, b, i, e) in relays:
                        relays[d, b, i, e].start()

    def settle(b, pieces):
        for (_, r, i, _), c in relays.items():
            if r == b and i in pieces:
                c.wait_recv()

    def windows(pairs, ids):
        return sum([list(range(pairs[i][0], sum(pairs[i]))) for i in ids], [])

    def gather(ref, ws):
        return jnp.concatenate([ref[w] for w in ws], axis=0)

    def block0(parts):
        st = {}
        parts = [(windows(heads_of, ids), ids) for ids in parts]
        ws = sum([p for p, _ in parts], [])

        def wait():
            pass

        def score():
            st["triple"] = project(gather(nq, ws), 0)
            st["scores"] = scores_of(st["triple"], hmask, heads)

        def soften():
            st["att"] = blend(weigh(st["scores"], bias[0], None), st["triple"], hmask, heads)

        def middle():
            st["mid"] = mix(gather(xq, ws).astype(f32), jnp.concatenate(st["att"], axis=0), 0)

        def close():
            mid, normed = st["mid"]
            start = 0
            for p, ids in parts:
                end = start + len(p) * KEYS
                y = feed(mid[start:end], normed[start:end], 0)
                for g, w in enumerate(p):
                    x1[w] = y[g * KEYS : (g + 1) * KEYS]
                start = end
                for i in ids:
                    halo(i).start()
                if 0 in p:
                    for c in edges:
                        c.start()

        return {"wait": wait, "score": score, "soften": soften, "middle": middle, "close": close}

    def own_half(ws):
        return sum([[x1[w, PART : 2 * PART], x1[w + 1, :PART]] for w in ws], [])

    def far_half(ws):
        return sum([[above[w, PART :], above[w + 1, :PART]] for w in ws], [])

    def masks(ws):
        return [jnp.broadcast_to(rt[:, w : w + 1], (KEYS, 128)) == ru[w : w + 1, :] for w in ws]

    def split_rows(x):
        return [x[i : i + 2 * PART] for i in range(0, x.shape[0], 2 * PART)]

    def block1(parts, halos):
        st = {}
        parts = [(windows(spans, ids), ids) for ids in parts]
        ws = sum([p for p, _ in parts], [])

        def wait():
            for c in halos:
                c.wait_recv()

        def score():
            mine, other = own_half(ws), far_half(ws)
            toks = []
            for g in range(0, 2 * len(ws), 2):
                toks += other[g : g + 2] + mine[g : g + 2]
            toks = jnp.concatenate(toks, axis=0).astype(f32)
            st["triple"] = project(layer_norm(toks, gain[1, 0:1], shift[1, 0:1]), 1)
            st["scores"] = scores_of(st["triple"], hmask, heads)

        def soften():
            outs = blend(weigh(st["scores"], bias[1], masks(ws)), st["triple"], hmask, heads)
            st["att"] = [o[: 2 * PART] for o in outs]
            for w, o in zip(ws, outs):
                att[w] = o[2 * PART :]

        def middle():
            x, y = far_half(ws), list(st["att"])
            if nwin - 1 in ws:
                x, y = x + own_half([nwin - 1]), y + [att[nwin - 1]]
            st["mid"] = mix(jnp.concatenate(x, axis=0).astype(f32), jnp.concatenate(y, axis=0), 1)

        def close():
            mid, normed = st["mid"]
            start = 0
            for p, ids in parts:
                tail = nwin - 1 in p
                end = start + (len(p) + tail) * 2 * PART
                ys = split_rows(feed(mid[start:end], normed[start:end], 1))
                for w, y in zip(p, ys):
                    yr[w] = y
                if tail:
                    yo[nwin] = ys[-1]
                start = end
                for i in ids:
                    back(i).start()
                if tail:
                    for c in fringe:
                        c.start()

        return {"wait": wait, "score": score, "soften": soften, "middle": middle, "close": close}

    def own(ws):
        x = jnp.concatenate(own_half(ws), axis=0).astype(f32)
        for w, y in zip(ws, split_rows(feed(*mix(x, gather(att, ws), 1), 1))):
            yo[w + 1] = y

    first = [block0([[0, 1], [2]])] + [block0([[i]]) for i in range(3, len(heads_of))]
    bring(0, (0,))
    settle(0, (0,))
    overlap(first[0], None)
    bring(0, (1, 2, 3))
    first[0]["middle"]()
    first[1]["score"]()
    settle(0, (1, 2, 3))
    first[0]["close"]()
    bring(1, range(4))
    first[1]["soften"]()
    for t in range(1, chunks):
        overlap(first[t + 1] if t < chunks - 1 else None, first[t])
    regions()
    settle(1, range(4))
    second = [block1([[0]], [halo(1), halo(2)] + edges)]
    second += [block1([[i]], [halo(i + 2)]) for i in range(1, chunks - 1)]
    second += [block1([[chunks - 1], [chunks]], [halo(0), halo(chunks + 1)])]
    overlap(second[0], None)
    pl.semaphore_wait(ready, 2)
    for t in range(1, chunks):
        overlap(second[t], second[t - 1])
    overlap(None, second[-1])
    half = nwin // 2
    own(list(range(half)))
    own(list(range(half, nwin - 1)))

    def place(src, base):
        v = src[...].astype(f32)
        for i in range(2):
            left, right = v[:nwin, PART + i * WIN : PART + (i + 1) * WIN], v[1:, i * WIN : (i + 1) * WIN]
            for r, y in enumerate(swap_halves(left, right)):
                o_ref[base + 2 * i + r] = y.reshape(cols, width).astype(bf16)

    fringe[0].wait_recv()
    place(yo, 0)
    for c in labels + smalls + edges + fringe + list(direct.values()) + list(relays.values()):
        c.wait_send()
    for i in range(len(heads_of)):
        halo(i).wait_send()
    for i in range(len(spans)):
        back(i).wait_send()
    for i in range(len(spans)):
        back(i).wait_recv()
    fringe[1].wait_recv()
    place(yt, SHIFT)


def on_device(*args):
    x = args[0]
    rows, cols, width = x.shape
    n = lax.axis_size("ch")
    heads = args[7].shape[2] * n
    args = list(args)
    args[5] = args[5].swapaxes(2, 3)
    args[6] = args[6].swapaxes(0, 1)
    args[7] = args[7].swapaxes(1, 2)
    hidden = args[10].shape[2] * n
    nwin = cols // WIN
    group = max(d for d in range(1, MOST + 1) if nwin % d == 0)
    chunks = nwin // group
    assert rows == WIN and heads % 2 == 0 and chunks > 1
    dma = pltpu.SemaphoreType.DMA
    vm = pltpu.VMEM
    scratch = [
        vm(x.shape, bf16), vm((rows, cols), i32), vm(args[2].shape, i32), vm(args[3].shape, f32),
        vm(args[4].shape, f32), vm(args[9].shape, f32), vm(args[13].shape, f32),
        vm((BLOCKS, 3, width, width), bf16), vm((BLOCKS, width, width), bf16),
        vm((BLOCKS, width, hidden), bf16), vm((BLOCKS, hidden, width), bf16),
        vm((n,) + args[7].shape, f32), vm((n,) + args[6].shape, f32), vm((n,) + args[11].shape, f32),
        vm((BLOCKS, 1, 3 * width), f32), vm((BLOCKS, 1, hidden), f32), vm((BLOCKS, KEYS, heads * KEYS), f32),
        vm((3, rows, cols), i32), vm((KEYS, 128), f32), vm((128, 128), f32),
        vm((nwin, KEYS, width), bf16), vm((nwin, KEYS, width), bf16), vm((nwin, 2 * PART, width), bf16),
        vm((nwin + 1, KEYS, width), bf16), vm((nwin + 1, 2 * PART, width), bf16),
        vm((nwin, 2 * PART, width), bf16), vm((nwin + 1, 2 * PART, width), bf16),
        vm((nwin + 1, 2 * PART, width), bf16),
        dma((14,)), dma((n - 1, 3)), dma((n - 1, 3)), dma((n - 1, BLOCKS, 4)), dma((n - 1, BLOCKS, 4)),
        dma((n - 1, BLOCKS, 4)), dma((n - 1, BLOCKS, 4)), dma((3,)), dma((3,)),
        dma((chunks + 2,)), dma((chunks + 2,)), dma((2,)), dma((2,)),
        dma((chunks + 1,)), dma((chunks + 1,)), dma((2,)), dma((2,)),
        pltpu.SemaphoreType.REGULAR,
    ]
    return pl.pallas_call(
        functools.partial(fused, heads, group),
        out_shape=vm(x.shape, bf16),
        in_specs=[pl.BlockSpec(memory_space=pl.ANY)] * len(args),
        out_specs=pl.BlockSpec(memory_space=vm),
        scratch_shapes=scratch,
        compiler_params=pltpu.CompilerParams(
            collective_id=0, has_side_effects=True, vmem_limit_bytes=56 * 1024 * 1024
        ),
        name="fused",
    )(*args)


def solution(mesh):
    in_specs = (
        P(("row", "ch"), "col", None), P(("row", "ch"), "col"), P(), P(), P(),
        P(None, None, None, "ch"), P(None, None, "ch"), P(None, None, "ch"), P(None, "ch", None), P(),
        P(None, None, "ch"), P(None, "ch"), P(None, "ch", None), P(),
    )
    out_specs = P(("row", "ch"), "col", None)
    return jax.shard_map(on_device, mesh=mesh, in_specs=in_specs, out_specs=out_specs, check_vma=False)
```

```python
import functools

import jax
import jax.numpy as jnp
from jax import lax
from jax.experimental import pallas as pl
from jax.experimental.pallas import tpu as pltpu
from jax.sharding import PartitionSpec as P

WIN = 8
SHIFT = 4
BLOCKS = 2
EPS = 1e-05
FAR = -1e30
LOG2E = 1.4426950408889634
MOST = 8
WHOLE = ((0, 1),)
ORDER = ("middle", "score", "close", "soften")
bf16 = jnp.bfloat16
f32 = jnp.float32
i32 = jnp.int32
KEYS = WIN * WIN
PART = SHIFT * SHIFT


def dot(a, b):
    return jnp.dot(a, b, preferred_element_type=f32)


def dot_t(a, b):
    return lax.dot_general(a, b, (((1,), (1,)), ((), ())), preferred_element_type=f32)


def layer_norm(x, gain, offset):
    center = x - jnp.mean(x, axis=-1, keepdims=True)
    spread = jnp.mean(center * center, axis=-1, keepdims=True)
    return (center * lax.rsqrt(spread + EPS) * gain + offset).astype(bf16)


def rows_of(x):
    return x.reshape(x.shape[0] * x.shape[1], x.shape[2])


def swap_halves(e, o):
    low = lax.broadcasted_iota(i32, e.shape, 1) < SHIFT
    return jnp.where(low, e, pltpu.roll(o, SHIFT, 1)), jnp.where(low, pltpu.roll(e, SHIFT, 1), o)


def quads(x):
    rows, wide, width = x.shape
    g = wide // WIN
    pairs = []
    for r in range(0, rows, 2):
        pairs.append(swap_halves(x[r].reshape(g, WIN, width), x[r + 1].reshape(g, WIN, width)))
    parts = []
    for w in range(g):
        for h in range(0, rows // 2, 2):
            parts += [pairs[h + i][s][w] for s in (0, 1) for i in (0, 1)]
    return jnp.concatenate(parts, axis=0)


def place_of(t):
    q, i = t >> 4, t & 15
    return SHIFT * (q >> 1) + (i >> 2), SHIFT * (q & 1) + (i & 3)


def head_mask(heads, keys, width):
    depth = width // heads
    row = lax.broadcasted_iota(i32, (heads * keys, width), 0) // keys
    col = lax.broadcasted_iota(i32, (heads * keys, width), 1) // depth
    return (row == col).astype(f32).astype(bf16)


def scores_of(triple, hmask, heads):
    width = triple.shape[1] // 3
    out = []
    for w in range(0, triple.shape[0], KEYS):
        q, k = triple[w : w + KEYS, :width], triple[w : w + KEYS, width : 2 * width]
        out.append(dot_t(q, jnp.concatenate([k] * heads, axis=0) * hmask))
    return out


def weigh(scores, bias, masks):
    low = lax.broadcasted_iota(i32, (bias.shape[0], 128), 1) < KEYS
    weights = []
    for w, s in enumerate(scores):
        parts = []
        for c in range(0, s.shape[1], 128):
            t = s[:, c : c + 128] + bias[:, c : c + 128]
            if masks is not None:
                t = jnp.where(masks[w], t, FAR)
            u = t.astype(bf16)
            first = jnp.max(jnp.where(low, u, bf16(-jnp.inf)), axis=-1, keepdims=True)
            second = jnp.max(jnp.where(low, bf16(-jnp.inf), u), axis=-1, keepdims=True)
            parts.append(jnp.exp2(t - jnp.where(low, first, second).astype(f32)))
        weights.append(jnp.concatenate(parts, axis=1).astype(bf16))
    return weights


def blend(weights, triple, hmask, heads):
    width = triple.shape[1] // 3
    outs = []
    for w, p in enumerate(weights):
        v = triple[w * KEYS : (w + 1) * KEYS, 2 * width :]
        o = dot(p, jnp.concatenate([jnp.concatenate([v] * heads, axis=0) * hmask, hmask], axis=1))
        outs.append((o[:, :width] / o[:, width:]).astype(bf16))
    return outs


def overlap(now, before):
    if now is not None:
        now["wait"]()
    for stage in ORDER:
        task = now if stage in ("score", "soften") else before
        if task is not None:
            task[stage]()


def fused(
    heads, group,
    x_h, lab_h, rel_h, gain_h, shift_h, qkvw_h, qkvb_h, table_h, projw_h, projb_h, fc1w_h, fc1b_h, fc2w_h, fc2b_h,
    o_ref,
    x_v, lab, rel, gain, shift, proj_b, fc2_b,
    qkv, proj, fc1, fc2, tab_all, qb_all, f1b_all, qb, f1b, bias, lab3, rt, ru,
    xq, nq, att, x1, above, yr, yt, yo,
    in_sem, extra, srecv, wsend, wrecv, rsend, rrecv, lsend, lrecv, hrecv, erecv, orecv, frecv, ready,
):
    rows, cols, width = x_v.shape
    nwin = cols // WIN
    chunks = nwin // group
    n = lax.axis_size("ch")
    nrow, ncol = lax.axis_size("row"), lax.axis_size("col")
    row, col, ch = lax.axis_index("row"), lax.axis_index("col"), lax.axis_index("ch")
    ring = row * n + ch
    total = nrow * n

    def at(dr, dc):
        p = lax.rem(ring + dr + total, total)
        return (p // n, lax.rem(col + dc + ncol, ncol), lax.rem(p, n))

    around = [(1, 0), (0, -1), (1, -1), (-1, 0), (0, 1), (-1, 1)]
    peers = [(row, col, lax.rem(ch + d, n)) for d in range(1, n)]
    mate = (row, col + 1 - 2 * lax.rem(col, 2), ch)
    core = lax.rem(col, 2)
    mesh_id = pl.DeviceIdType.MESH

    barrier = pltpu.get_barrier_semaphore()
    targets = [at(*d) for d in around[3:]] + peers + [mate]
    for t in targets:
        pl.semaphore_signal(barrier, inc=1, device_id=t, device_id_type=mesh_id)

    def remote(src, dst, ssem, rsem, to):
        return pltpu.make_async_remote_copy(
            src_ref=src, dst_ref=dst, send_sem=ssem, recv_sem=rsem, device_id=to, device_id_type=mesh_id
        )

    part, pw, fw, gw = width // n, projw_h.shape[1], fc1w_h.shape[2], fc2w_h.shape[1]

    def slots(b, owner, share, count):
        out = []
        for i, size in enumerate((part, pw, width, gw)):
            start = owner * size if i != 2 else 0
            if (b, i) not in WHOLE:
                size = size // count
                start = start + share * size
            span = pl.ds(pl.multiple_of(start, 16), size)
            lanes = pl.ds(pl.multiple_of(owner * fw, 128), fw)
            out.append((
                lambda: qkv.at[b, :, span, :], lambda: proj.at[b, span, :],
                lambda: fc1.at[b, span, lanes], lambda: fc2.at[b, span, :],
            )[i]())
        return out

    loads = {}
    for i, (name, s, d) in enumerate([
        ("table", table_h, tab_all.at[ch]), ("qb", qkvb_h, qb_all.at[ch]), ("f1b", fc1b_h, f1b_all.at[ch]),
        ("qkv", qkvw_h, qkv.at[:, :, pl.ds(pl.multiple_of(ch * part, 16), part), :]),
        ("proj", projw_h, proj.at[:, pl.ds(pl.multiple_of(ch * pw, 16), pw), :]),
        ("fc1", fc1w_h, fc1.at[:, :, pl.ds(pl.multiple_of(ch * fw, 128), fw)]),
        ("fc2", fc2w_h, fc2.at[:, pl.ds(pl.multiple_of(ch * gw, 16), gw), :]),
        ("lab", lab_h, lab), ("x", x_h, x_v), ("gain", gain_h, gain), ("shift", shift_h, shift),
        ("rel", rel_h, rel), ("proj_b", projb_h, proj_b), ("fc2_b", fc2b_h, fc2_b),
    ]):
        loads[name] = pltpu.make_async_copy(s, d, in_sem.at[i])
        loads[name].start()
    pl.semaphore_wait(barrier, len(targets))
    for d in (around[0], around[2]):
        pl.semaphore_signal(ready, inc=1, device_id=at(*d), device_id_type=mesh_id)

    shares = {b: (core, 2, [mate]) for b in range(BLOCKS)}
    direct, relays, smalls = {}, {}, []
    for d in range(1, n):
        to, owner = peers[d - 1], lax.rem(ch - d + n, n)
        for b in range(BLOCKS):
            share, count, others = shares[b]
            for i, s in enumerate(slots(b, ch, share, count)):
                sent = wsend.at[d - 1, i] if b else in_sem.at[3 + i] if d == 1 else extra.at[7 * (d - 2) + 3 + i]
                direct[d, b, i] = remote(s, s, sent, wrecv.at[d - 1, b, i], to)
            for e, other in enumerate(others):
                for i, s in enumerate(slots(b, owner, share, count)):
                    if (b, i) not in WHOLE:
                        r = b + e
                        relays[d, b, i, e] = remote(s, s, rsend.at[d - 1, r, i], rrecv.at[d - 1, r, i], other)
        for i, ref in enumerate([tab_all, qb_all, f1b_all]):
            sent = in_sem.at[i] if d == 1 else extra.at[7 * (d - 2) + i]
            smalls.append(remote(ref.at[ch], ref.at[ch], sent, srecv.at[d - 1, i], to))
    loads["lab"].wait()
    labels = []
    for i, d in enumerate(around[:3]):
        labels.append(remote(lab, lab3.at[i], lsend.at[i], lrecv.at[i], at(*d)))
        labels[-1].start()
    for name in ("table", "qb", "f1b", "qkv", "proj", "fc1", "fc2"):
        loads[name].wait()
    for c in smalls:
        c.start()
    for b in range(BLOCKS):
        for i in range(4):
            for d in range(1, n):
                direct[d, b, i].start()
    for name in ("x", "gain", "shift", "rel", "proj_b", "fc2_b"):
        loads[name].wait()

    def here(k, more=0):
        return pl.ds(k * group, group + more)

    def prepare(k, _):
        t = quads(x_v[:, pl.ds(pl.multiple_of(k * group * WIN, WIN), group * WIN), :].astype(f32))
        xq[here(k)] = t.astype(bf16).reshape(group, KEYS, width)
        nq[here(k)] = layer_norm(t, gain[0, 0:1], shift[0, 0:1]).reshape(group, KEYS, width)
        return 0

    lax.fori_loop(0, chunks, prepare, 0)

    idx = quads(jnp.concatenate([rel[...]] * 2, axis=1).reshape(WIN, WIN, 128))
    lane = lax.broadcasted_iota(i32, (KEYS, 128), 1)
    a, c = place_of(lane & (KEYS - 1))
    idx = jnp.take_along_axis(idx, (lane & KEYS) + a * WIN + c, axis=1, mode="promise_in_bounds")
    for c in smalls:
        c.wait_recv()
    scale = (width // heads) ** (-0.5) * LOG2E
    for j in range(n):
        for b in range(BLOCKS):
            for m in range(3):
                qb[b, :, m * width + j * part : m * width + (j + 1) * part] = qb_all[j, m, b : b + 1, :]
            f1b[b, :, j * fw : (j + 1) * fw] = f1b_all[j, b : b + 1, :]
    local_heads, entries = table_h.shape[1:]
    for b in range(BLOCKS):
        for t in range(heads // 2):
            out = []
            for h in (2 * t, 2 * t + 1):
                entry = tab_all[h // local_heads, b, h % local_heads : h % local_heads + 1, :]
                got = None
                for c in range(0, entries, 128):
                    piece = entry[:, c : c + 128]
                    if piece.shape[1] < 128:
                        piece = jnp.concatenate([piece, jnp.zeros((1, 128 - piece.shape[1]), f32)], axis=1)
                    piece = jnp.broadcast_to(piece, idx.shape)
                    piece = jnp.take_along_axis(piece, idx & 127, axis=1, mode="promise_in_bounds")
                    got = piece if got is None else jnp.where(idx >= c, piece, got)
                out.append(got)
            bias[b, :, t * 128 : (t + 1) * 128] = jnp.where(lane < KEYS, out[0], out[1]) * LOG2E

    hmask = head_mask(heads, KEYS, width)

    def project(normed, b):
        out = dot_t(normed, rows_of(qkv[b])) + qb[b]
        return jnp.concatenate([(out[:, :width] * scale).astype(bf16), out[:, width:].astype(bf16)], axis=1)

    def regions():
        for c in labels:
            c.wait_recv()
        kind = jnp.concatenate([lab3[0, SHIFT:], lab[:SHIFT]], axis=0).astype(f32)
        kind = pltpu.roll(kind, cols - SHIFT, 1)
        wrap = jnp.concatenate([lab3[2, SHIFT:, :128], lab3[1, :SHIFT, :128]], axis=0).astype(f32)
        wrap = jnp.concatenate([jnp.zeros((rows, cols - 128), f32), pltpu.roll(wrap, 128 - SHIFT, 1)], axis=1)
        i = lax.broadcasted_iota(i32, (rows, cols), 0)
        j = lax.broadcasted_iota(i32, (rows, cols), 1)
        def flag(where, when):
            return jnp.where(where, when.astype(f32), 0.0)
        kind = jnp.where(j >= cols - SHIFT, wrap, kind) * 4.0
        kind = kind + flag(i >= SHIFT, ring == 0) * 2.0 + flag(j >= cols - SHIFT, col == ncol - 1)
        lane8 = lax.broadcasted_iota(i32, (rows, 128), 1)
        per = 128 // WIN
        stack = []
        for c in range(WIN):
            got = None
            for p in range(0, cols, 128):
                piece = jnp.take_along_axis(
                    kind[:, p : p + 128], (lane8 & (per - 1)) * WIN + c, axis=1, mode="promise_in_bounds"
                )
                got = piece if got is None else jnp.where(lane8 >= p // WIN, piece, got)
            stack.append(got)
        stack = jnp.concatenate(stack, axis=0).astype(bf16)
        a, c = place_of(lax.broadcasted_iota(i32, (128, KEYS), 0) & (KEYS - 1))
        pick = (c * WIN + a == lax.broadcasted_iota(i32, (128, KEYS), 1)).astype(f32).astype(bf16)
        kinds = dot(pick, stack)
        ru[...] = kinds.T
        rt[...] = kinds[:KEYS]

    def mix(x, attended, b):
        middle = (x + dot(attended, proj[b]) + proj_b[b : b + 1]).astype(bf16).astype(f32)
        return middle, layer_norm(middle, gain[b, 1:2], shift[b, 1:2])

    def widen(normed, b):
        inner = (dot(normed, fc1[b]) + f1b[b]).astype(bf16)
        return inner * (lax.erf(inner * bf16(0.5 ** 0.5)) + bf16(1.0))

    def narrow(middle, hidden, b):
        outer = dot(hidden, fc2[b] * bf16(0.5))
        return (middle + outer + fc2_b[b : b + 1]).astype(bf16)

    def feed(middle, normed, b):
        return narrow(middle, widen(normed, b), b)

    cut = group // 2
    final = nwin - group
    heads_of = [(0, 1), (final, cut), (final + cut, group - cut)]
    heads_of += [(k * group, group) for k in range(chunks - 2, 0, -1)] + [(1, group - 1)]

    def halo(i):
        start, size = heads_of[i]
        span = pl.ds(start, size)
        return remote(x1.at[span, 2 * PART :, :], above.at[span], in_sem.at[8 + i], hrecv.at[i], at(1, 0))

    edges = [
        remote(x1.at[0, :PART], x1.at[nwin, :PART], lsend.at[0], erecv.at[0], at(0, -1)),
        remote(x1.at[0, 2 * PART : 3 * PART], above.at[nwin, :PART], lsend.at[1], erecv.at[1], at(1, -1)),
    ]

    spans = [(k * group, group) for k in range(chunks - 1, 0, -1)] + [(0, cut), (cut, group - cut)]

    def back(i):
        start, size = spans[i]
        return remote(
            yr.at[pl.ds(start, size)], yt.at[pl.ds(start + 1, size)], in_sem.at[i], orecv.at[i], at(-1, 0)
        )

    fringe = [
        remote(yo.at[nwin, PART :], yo.at[0, PART :], in_sem.at[chunks + 1], frecv.at[0], at(0, 1)),
        remote(yr.at[nwin - 1, PART :], yt.at[0, PART :], in_sem.at[chunks + 2], frecv.at[1], at(-1, 1)),
    ]

    def bring(b, pieces):
        for i in pieces:
            for d in range(1, n):
                direct[d, b, i].wait_recv()
                for e in range(len(shares[b][2])):
                    if (d, b, i, e) in relays:
                        relays[d, b, i, e].start()

    def settle(b, pieces):
        for (_, r, i, _), c in relays.items():
            if r == b and i in pieces:
                c.wait_recv()

    def windows(pairs, ids):
        return sum([list(range(pairs[i][0], sum(pairs[i]))) for i in ids], [])

    def gather(ref, ws):
        return jnp.concatenate([ref[w] for w in ws], axis=0)

    def block0(parts):
        st = {}
        parts = [(windows(heads_of, ids), ids) for ids in parts]
        ws = sum([p for p, _ in parts], [])

        def wait():
            pass

        def score():
            st["triple"] = project(gather(nq, ws), 0)
            st["scores"] = scores_of(st["triple"], hmask, heads)

        def soften():
            st["att"] = blend(weigh(st["scores"], bias[0], None), st["triple"], hmask, heads)

        def middle():
            st["mid"] = mix(gather(xq, ws).astype(f32), jnp.concatenate(st["att"], axis=0), 0)

        def expand():
            st["hidden"] = widen(st["mid"][1], 0)

        def close():
            mid = st["mid"][0]
            if "hidden" not in st:
                expand()
            start = 0
            for p, ids in parts:
                end = start + len(p) * KEYS
                y = narrow(mid[start:end], st["hidden"][start:end], 0)
                for g, w in enumerate(p):
                    x1[w] = y[g * KEYS : (g + 1) * KEYS]
                start = end
                for i in ids:
                    halo(i).start()
                if 0 in p:
                    for c in edges:
                        c.start()

        return {
            "wait": wait, "score": score, "soften": soften, "middle": middle, "expand": expand, "close": close,
        }

    def own_half(ws):
        return sum([[x1[w, PART : 2 * PART], x1[w + 1, :PART]] for w in ws], [])

    def far_half(ws):
        return sum([[above[w, PART :], above[w + 1, :PART]] for w in ws], [])

    def masks(ws):
        return [jnp.broadcast_to(rt[:, w : w + 1], (KEYS, 128)) == ru[w : w + 1, :] for w in ws]

    def split_rows(x):
        return [x[i : i + 2 * PART] for i in range(0, x.shape[0], 2 * PART)]

    def block1(parts, halos):
        st = {}
        parts = [(windows(spans, ids), ids) for ids in parts]
        ws = sum([p for p, _ in parts], [])

        def wait():
            for c in halos:
                c.wait_recv()

        def score():
            mine, other = own_half(ws), far_half(ws)
            toks = []
            for g in range(0, 2 * len(ws), 2):
                toks += other[g : g + 2] + mine[g : g + 2]
            toks = jnp.concatenate(toks, axis=0).astype(f32)
            st["triple"] = project(layer_norm(toks, gain[1, 0:1], shift[1, 0:1]), 1)
            st["scores"] = scores_of(st["triple"], hmask, heads)

        def soften():
            outs = blend(weigh(st["scores"], bias[1], masks(ws)), st["triple"], hmask, heads)
            st["att"] = [o[: 2 * PART] for o in outs]
            for w, o in zip(ws, outs):
                att[w] = o[2 * PART :]

        def middle():
            x, y = far_half(ws), list(st["att"])
            if nwin - 1 in ws:
                x, y = x + own_half([nwin - 1]), y + [att[nwin - 1]]
            st["mid"] = mix(jnp.concatenate(x, axis=0).astype(f32), jnp.concatenate(y, axis=0), 1)

        def close():
            mid, normed = st["mid"]
            start = 0
            for p, ids in parts:
                tail = nwin - 1 in p
                end = start + (len(p) + tail) * 2 * PART
                ys = split_rows(feed(mid[start:end], normed[start:end], 1))
                for w, y in zip(p, ys):
                    yr[w] = y
                if tail:
                    yo[nwin] = ys[-1]
                start = end
                for i in ids:
                    back(i).start()
                if tail:
                    for c in fringe:
                        c.start()

        return {"wait": wait, "score": score, "soften": soften, "middle": middle, "close": close}

    def own(ws):
        x = jnp.concatenate(own_half(ws), axis=0).astype(f32)
        for w, y in zip(ws, split_rows(feed(*mix(x, gather(att, ws), 1), 1))):
            yo[w + 1] = y

    first = [block0([[0, 1], [2]])] + [block0([[i]]) for i in range(3, len(heads_of))]
    bring(0, (0,))
    settle(0, (0,))
    first[0]["score"]()
    bring(0, (1, 2))
    first[0]["soften"]()
    bring(0, (3,))
    first[0]["middle"]()
    settle(0, (2,))
    first[0]["expand"]()
    first[1]["score"]()
    for c in labels:
        c.wait_send()
    settle(0, (3,))
    first[0]["close"]()
    bring(1, range(4))
    first[1]["soften"]()
    for t in range(1, chunks):
        overlap(first[t + 1] if t < chunks - 1 else None, first[t])
    regions()
    settle(1, range(4))
    second = [block1([[0]], [halo(1), halo(2)] + edges)]
    second += [block1([[i]], [halo(i + 2)]) for i in range(1, chunks - 1)]
    second += [block1([[chunks - 1], [chunks]], [halo(0), halo(chunks + 1)])]
    overlap(second[0], None)
    pl.semaphore_wait(ready, 2)
    for c in smalls + [c for (_, b, _), c in direct.items() if b == 0]:
        c.wait_send()
    own(list(range(final, nwin - 1)))
    for t in range(1, chunks):
        overlap(second[t], second[t - 1])
    overlap(None, second[-1])
    half = nwin // 2
    own(list(range(final)))

    def place(src, base):
        v = src[...].astype(f32)
        for i in range(2):
            left, right = v[:nwin, PART + i * WIN : PART + (i + 1) * WIN], v[1:, i * WIN : (i + 1) * WIN]
            for r, y in enumerate(swap_halves(left, right)):
                o_ref[base + 2 * i + r] = y.reshape(cols, width).astype(bf16)

    fringe[0].wait_recv()
    place(yo, 0)
    for c in edges + fringe + [c for (_, b, _), c in direct.items() if b] + list(relays.values()):
        c.wait_send()
    for i in range(len(heads_of)):
        halo(i).wait_send()
    for i in range(len(spans)):
        back(i).wait_send()
    for i in range(len(spans)):
        back(i).wait_recv()
    fringe[1].wait_recv()
    place(yt, SHIFT)


def on_device(*args):
    x = args[0]
    rows, cols, width = x.shape
    n = lax.axis_size("ch")
    heads = args[7].shape[2] * n
    args = list(args)
    args[5] = args[5].swapaxes(2, 3)
    args[6] = args[6].swapaxes(0, 1)
    args[7] = args[7].swapaxes(1, 2)
    hidden = args[10].shape[2] * n
    nwin = cols // WIN
    group = max(d for d in range(1, MOST + 1) if nwin % d == 0)
    chunks = nwin // group
    assert rows == WIN and heads % 2 == 0 and chunks > 1
    dma = pltpu.SemaphoreType.DMA
    vm = pltpu.VMEM
    scratch = [
        vm(x.shape, bf16), vm((rows, cols), i32), vm(args[2].shape, i32), vm(args[3].shape, f32),
        vm(args[4].shape, f32), vm(args[9].shape, f32), vm(args[13].shape, f32),
        vm((BLOCKS, 3, width, width), bf16), vm((BLOCKS, width, width), bf16),
        vm((BLOCKS, width, hidden), bf16), vm((BLOCKS, hidden, width), bf16),
        vm((n,) + args[7].shape, f32), vm((n,) + args[6].shape, f32), vm((n,) + args[11].shape, f32),
        vm((BLOCKS, 1, 3 * width), f32), vm((BLOCKS, 1, hidden), f32), vm((BLOCKS, KEYS, heads * KEYS), f32),
        vm((3, rows, cols), i32), vm((KEYS, 128), f32), vm((128, 128), f32),
        vm((nwin, KEYS, width), bf16), vm((nwin, KEYS, width), bf16), vm((nwin, 2 * PART, width), bf16),
        vm((nwin + 1, KEYS, width), bf16), vm((nwin + 1, 2 * PART, width), bf16),
        vm((nwin, 2 * PART, width), bf16), vm((nwin + 1, 2 * PART, width), bf16),
        vm((nwin + 1, 2 * PART, width), bf16),
        dma((10 + max(4, chunks),)), dma((max(1, 7 * (n - 2)),)), dma((n - 1, 3)), dma((n - 1, 4)), dma((n - 1, BLOCKS, 4)),
        dma((n - 1, BLOCKS, 4)), dma((n - 1, BLOCKS, 4)), dma((3,)), dma((3,)),
        dma((chunks + 2,)), dma((2,)), dma((chunks + 1,)), dma((2,)),
        pltpu.SemaphoreType.REGULAR,
    ]
    return pl.pallas_call(
        functools.partial(fused, heads, group),
        out_shape=vm(x.shape, bf16),
        in_specs=[pl.BlockSpec(memory_space=pl.ANY)] * len(args),
        out_specs=pl.BlockSpec(memory_space=vm),
        scratch_shapes=scratch,
        compiler_params=pltpu.CompilerParams(
            collective_id=0, has_side_effects=True, vmem_limit_bytes=56 * 1024 * 1024
        ),
        name="fused",
    )(*args)


def solution(mesh):
    in_specs = (
        P(("row", "ch"), "col", None), P(("row", "ch"), "col"), P(), P(), P(),
        P(None, None, None, "ch"), P(None, None, "ch"), P(None, None, "ch"), P(None, "ch", None), P(),
        P(None, None, "ch"), P(None, "ch"), P(None, "ch", None), P(),
    )
    out_specs = P(("row", "ch"), "col", None)
    return jax.shard_map(on_device, mesh=mesh, in_specs=in_specs, out_specs=out_specs, check_vma=False)
```

```python
import functools

import jax
import jax.numpy as jnp
from jax import lax
from jax.experimental import pallas as pl
from jax.experimental.pallas import tpu as pltpu
from jax.sharding import PartitionSpec as P

WIN = 8
SHIFT = 4
BLOCKS = 2
EPS = 1e-05
FAR = -1e30
LOG2E = 1.4426950408889634
MOST = 8
WHOLE = ((0, 1),)
ORDER = ("middle", "score", "close", "soften")
bf16 = jnp.bfloat16
f32 = jnp.float32
i32 = jnp.int32
KEYS = WIN * WIN
PART = SHIFT * SHIFT


def dot(a, b):
    return jnp.dot(a, b, preferred_element_type=f32)


def dot_t(a, b):
    return lax.dot_general(a, b, (((1,), (1,)), ((), ())), preferred_element_type=f32)


def layer_norm(x, gain, offset):
    center = x - jnp.mean(x, axis=-1, keepdims=True)
    spread = jnp.mean(center * center, axis=-1, keepdims=True)
    return (center * lax.rsqrt(spread + EPS) * gain + offset).astype(bf16)


def rows_of(x):
    return x.reshape(x.shape[0] * x.shape[1], x.shape[2])


def swap_halves(e, o):
    low = lax.broadcasted_iota(i32, e.shape, 1) < SHIFT
    return jnp.where(low, e, pltpu.roll(o, SHIFT, 1)), jnp.where(low, pltpu.roll(e, SHIFT, 1), o)


def quads(x):
    rows, wide, width = x.shape
    g = wide // WIN
    pairs = []
    for r in range(0, rows, 2):
        pairs.append(swap_halves(x[r].reshape(g, WIN, width), x[r + 1].reshape(g, WIN, width)))
    parts = []
    for w in range(g):
        for h in range(0, rows // 2, 2):
            parts += [pairs[h + i][s][w] for s in (0, 1) for i in (0, 1)]
    return jnp.concatenate(parts, axis=0)


def place_of(t):
    q, i = t >> 4, t & 15
    return SHIFT * (q >> 1) + (i >> 2), SHIFT * (q & 1) + (i & 3)


def head_mask(heads, keys, width):
    depth = width // heads
    row = lax.broadcasted_iota(i32, (heads * keys, width), 0) // keys
    col = lax.broadcasted_iota(i32, (heads * keys, width), 1) // depth
    return (row == col).astype(f32).astype(bf16)


def scores_of(triple, hmask, heads):
    width = triple.shape[1] // 3
    out = []
    for w in range(0, triple.shape[0], KEYS):
        q, k = triple[w : w + KEYS, :width], triple[w : w + KEYS, width : 2 * width]
        out.append(dot_t(q, jnp.concatenate([k] * heads, axis=0) * hmask))
    return out


def weigh(scores, bias, masks):
    low = lax.broadcasted_iota(i32, (bias.shape[0], 128), 1) < KEYS
    weights = []
    for w, s in enumerate(scores):
        parts = []
        for c in range(0, s.shape[1], 128):
            t = s[:, c : c + 128] + bias[:, c : c + 128]
            if masks is not None:
                t = jnp.where(masks[w], t, FAR)
            u = t.astype(bf16)
            first = jnp.max(jnp.where(low, u, bf16(-jnp.inf)), axis=-1, keepdims=True)
            second = jnp.max(jnp.where(low, bf16(-jnp.inf), u), axis=-1, keepdims=True)
            parts.append(jnp.exp2(t - jnp.where(low, first, second).astype(f32)))
        weights.append(jnp.concatenate(parts, axis=1).astype(bf16))
    return weights


def blend(weights, triple, hmask, heads):
    width = triple.shape[1] // 3
    outs = []
    for w, p in enumerate(weights):
        v = triple[w * KEYS : (w + 1) * KEYS, 2 * width :]
        o = dot(p, jnp.concatenate([jnp.concatenate([v] * heads, axis=0) * hmask, hmask], axis=1))
        outs.append((o[:, :width] / o[:, width:]).astype(bf16))
    return outs


def overlap(now, before):
    if now is not None:
        now["wait"]()
    for stage in ORDER:
        task = now if stage in ("score", "soften") else before
        if task is not None:
            task[stage]()


def fused(
    heads, group,
    x_h, lab_h, rel_h, gain_h, shift_h, qkvw_h, qkvb_h, table_h, projw_h, projb_h, fc1w_h, fc1b_h, fc2w_h, fc2b_h,
    o_ref,
    x_v, lab, rel, gain, shift, proj_b, fc2_b,
    qkv, proj, fc1, fc2, tab_all, qb_all, f1b_all, qb, f1b, bias, lab3, rt, ru,
    xq, nq, att, x1, above, yr, yt, yo,
    in_sem, extra, srecv, wsend, wrecv, rsend, rrecv, lsend, lrecv, hrecv, erecv, orecv, frecv, ready,
):
    rows, cols, width = x_v.shape
    nwin = cols // WIN
    chunks = nwin // group
    n = lax.axis_size("ch")
    nrow, ncol = lax.axis_size("row"), lax.axis_size("col")
    row, col, ch = lax.axis_index("row"), lax.axis_index("col"), lax.axis_index("ch")
    ring = row * n + ch
    total = nrow * n

    def at(dr, dc):
        p = lax.rem(ring + dr + total, total)
        return (p // n, lax.rem(col + dc + ncol, ncol), lax.rem(p, n))

    around = [(1, 0), (0, -1), (1, -1), (-1, 0), (0, 1), (-1, 1)]
    peers = [(row, col, lax.rem(ch + d, n)) for d in range(1, n)]
    mate = (row, col + 1 - 2 * lax.rem(col, 2), ch)
    core = lax.rem(col, 2)
    mesh_id = pl.DeviceIdType.MESH

    barrier = pltpu.get_barrier_semaphore()
    targets = [at(*d) for d in around[3:]] + peers + [mate]
    for t in targets:
        pl.semaphore_signal(barrier, inc=1, device_id=t, device_id_type=mesh_id)

    def remote(src, dst, ssem, rsem, to):
        return pltpu.make_async_remote_copy(
            src_ref=src, dst_ref=dst, send_sem=ssem, recv_sem=rsem, device_id=to, device_id_type=mesh_id
        )

    part, pw, fw, gw = width // n, projw_h.shape[1], fc1w_h.shape[2], fc2w_h.shape[1]

    def slots(b, owner, share, count):
        out = []
        for i, size in enumerate((part, pw, width, gw)):
            start = owner * size if i != 2 else 0
            if (b, i) not in WHOLE:
                size = size // count
                start = start + share * size
            span = pl.ds(pl.multiple_of(start, 16), size)
            lanes = pl.ds(pl.multiple_of(owner * fw, 128), fw)
            out.append((
                lambda: qkv.at[b, :, span, :], lambda: proj.at[b, span, :],
                lambda: fc1.at[b, span, lanes], lambda: fc2.at[b, span, :],
            )[i]())
        return out

    loads = {}
    for i, (name, s, d) in enumerate([
        ("table", table_h, tab_all.at[ch]), ("qb", qkvb_h, qb_all.at[ch]), ("f1b", fc1b_h, f1b_all.at[ch]),
        ("qkv", qkvw_h, qkv.at[:, :, pl.ds(pl.multiple_of(ch * part, 16), part), :]),
        ("proj", projw_h, proj.at[:, pl.ds(pl.multiple_of(ch * pw, 16), pw), :]),
        ("fc1", fc1w_h, fc1.at[:, :, pl.ds(pl.multiple_of(ch * fw, 128), fw)]),
        ("fc2", fc2w_h, fc2.at[:, pl.ds(pl.multiple_of(ch * gw, 16), gw), :]),
        ("lab", lab_h, lab), ("x", x_h, x_v), ("gain", gain_h, gain), ("shift", shift_h, shift),
        ("rel", rel_h, rel), ("proj_b", projb_h, proj_b), ("fc2_b", fc2b_h, fc2_b),
    ]):
        loads[name] = pltpu.make_async_copy(s, d, in_sem.at[i])
        loads[name].start()
    pl.semaphore_wait(barrier, len(targets))
    for d in (around[0], around[2]):
        pl.semaphore_signal(ready, inc=1, device_id=at(*d), device_id_type=mesh_id)

    shares = {b: (core, 2, [mate]) for b in range(BLOCKS)}
    direct, relays, smalls = {}, {}, []
    for d in range(1, n):
        to, owner = peers[d - 1], lax.rem(ch - d + n, n)
        for b in range(BLOCKS):
            share, count, others = shares[b]
            for i, s in enumerate(slots(b, ch, share, count)):
                sent = wsend.at[d - 1, i] if b else in_sem.at[3 + i] if d == 1 else extra.at[7 * (d - 2) + 3 + i]
                direct[d, b, i] = remote(s, s, sent, wrecv.at[d - 1, b, i], to)
            for e, other in enumerate(others):
                for i, s in enumerate(slots(b, owner, share, count)):
                    if (b, i) not in WHOLE:
                        r = b + e
                        relays[d, b, i, e] = remote(s, s, rsend.at[d - 1, r, i], rrecv.at[d - 1, r, i], other)
        for i, ref in enumerate([tab_all, qb_all, f1b_all]):
            sent = in_sem.at[i] if d == 1 else extra.at[7 * (d - 2) + i]
            smalls.append(remote(ref.at[ch], ref.at[ch], sent, srecv.at[d - 1, i], to))
    loads["lab"].wait()
    labels = []
    for i, d in enumerate(around[:3]):
        labels.append(remote(lab, lab3.at[i], lsend.at[i], lrecv.at[i], at(*d)))
        labels[-1].start()
    for name in ("table", "qb", "f1b", "qkv", "proj", "fc1", "fc2"):
        loads[name].wait()
    for c in smalls:
        c.start()
    for b in range(BLOCKS):
        for i in range(4):
            for d in range(1, n):
                direct[d, b, i].start()
    for name in ("x", "gain", "shift", "rel", "proj_b", "fc2_b"):
        loads[name].wait()

    def here(k, more=0):
        return pl.ds(k * group, group + more)

    def prepare(k, _):
        t = quads(x_v[:, pl.ds(pl.multiple_of(k * group * WIN, WIN), group * WIN), :].astype(f32))
        xq[here(k)] = t.astype(bf16).reshape(group, KEYS, width)
        nq[here(k)] = layer_norm(t, gain[0, 0:1], shift[0, 0:1]).reshape(group, KEYS, width)
        return 0

    lax.fori_loop(0, chunks, prepare, 0)

    idx = quads(jnp.concatenate([rel[...]] * 2, axis=1).reshape(WIN, WIN, 128))
    lane = lax.broadcasted_iota(i32, (KEYS, 128), 1)
    a, c = place_of(lane & (KEYS - 1))
    idx = jnp.take_along_axis(idx, (lane & KEYS) + a * WIN + c, axis=1, mode="promise_in_bounds")
    for c in smalls:
        c.wait_recv()
    scale = (width // heads) ** (-0.5) * LOG2E
    for j in range(n):
        for b in range(BLOCKS):
            for m in range(3):
                qb[b, :, m * width + j * part : m * width + (j + 1) * part] = qb_all[j, m, b : b + 1, :]
            f1b[b, :, j * fw : (j + 1) * fw] = f1b_all[j, b : b + 1, :]
    local_heads, entries = table_h.shape[1:]
    for b in range(BLOCKS):
        for t in range(heads // 2):
            out = []
            for h in (2 * t, 2 * t + 1):
                entry = tab_all[h // local_heads, b, h % local_heads : h % local_heads + 1, :]
                got = None
                for c in range(0, entries, 128):
                    piece = entry[:, c : c + 128]
                    if piece.shape[1] < 128:
                        piece = jnp.concatenate([piece, jnp.zeros((1, 128 - piece.shape[1]), f32)], axis=1)
                    piece = jnp.broadcast_to(piece, idx.shape)
                    piece = jnp.take_along_axis(piece, idx & 127, axis=1, mode="promise_in_bounds")
                    got = piece if got is None else jnp.where(idx >= c, piece, got)
                out.append(got)
            bias[b, :, t * 128 : (t + 1) * 128] = jnp.where(lane < KEYS, out[0], out[1]) * LOG2E

    hmask = head_mask(heads, KEYS, width)

    def project(normed, b):
        out = dot_t(normed, rows_of(qkv[b])) + qb[b]
        return jnp.concatenate([(out[:, :width] * scale).astype(bf16), out[:, width:].astype(bf16)], axis=1)

    def regions():
        for c in labels:
            c.wait_recv()
        kind = jnp.concatenate([lab3[0, SHIFT:], lab[:SHIFT]], axis=0).astype(f32)
        kind = pltpu.roll(kind, cols - SHIFT, 1)
        wrap = jnp.concatenate([lab3[2, SHIFT:, :128], lab3[1, :SHIFT, :128]], axis=0).astype(f32)
        wrap = jnp.concatenate([jnp.zeros((rows, cols - 128), f32), pltpu.roll(wrap, 128 - SHIFT, 1)], axis=1)
        i = lax.broadcasted_iota(i32, (rows, cols), 0)
        j = lax.broadcasted_iota(i32, (rows, cols), 1)
        def flag(where, when):
            return jnp.where(where, when.astype(f32), 0.0)
        kind = jnp.where(j >= cols - SHIFT, wrap, kind) * 4.0
        kind = kind + flag(i >= SHIFT, ring == 0) * 2.0 + flag(j >= cols - SHIFT, col == ncol - 1)
        lane8 = lax.broadcasted_iota(i32, (rows, 128), 1)
        per = 128 // WIN
        stack = []
        for c in range(WIN):
            got = None
            for p in range(0, cols, 128):
                piece = jnp.take_along_axis(
                    kind[:, p : p + 128], (lane8 & (per - 1)) * WIN + c, axis=1, mode="promise_in_bounds"
                )
                got = piece if got is None else jnp.where(lane8 >= p // WIN, piece, got)
            stack.append(got)
        stack = jnp.concatenate(stack, axis=0).astype(bf16)
        a, c = place_of(lax.broadcasted_iota(i32, (128, KEYS), 0) & (KEYS - 1))
        pick = (c * WIN + a == lax.broadcasted_iota(i32, (128, KEYS), 1)).astype(f32).astype(bf16)
        kinds = dot(pick, stack)
        ru[...] = kinds.T
        rt[...] = kinds[:KEYS]

    def mix(x, attended, b):
        middle = (x + dot(attended, proj[b]) + proj_b[b : b + 1])
        return middle, layer_norm(middle, gain[b, 1:2], shift[b, 1:2])

    def widen(normed, b):
        inner = dot(normed, fc1[b]).astype(bf16) + f1b[b].astype(bf16)
        return inner * (lax.erf(inner * bf16(0.5 ** 0.5)) + bf16(1.0))

    def narrow(middle, hidden, b):
        outer = dot(hidden, fc2[b] * bf16(0.5))
        return (middle + outer + fc2_b[b : b + 1]).astype(bf16)

    def feed(middle, normed, b):
        return narrow(middle, widen(normed, b), b)

    cut = group // 2
    final = nwin - group
    heads_of = [(0, 1), (final, cut), (final + cut, group - cut)]
    heads_of += [(k * group, group) for k in range(chunks - 2, 0, -1)] + [(1, group - 1)]

    def halo(i):
        start, size = heads_of[i]
        span = pl.ds(start, size)
        return remote(x1.at[span, 2 * PART :, :], above.at[span], in_sem.at[8 + i], hrecv.at[i], at(1, 0))

    edges = [
        remote(x1.at[0, :PART], x1.at[nwin, :PART], lsend.at[0], erecv.at[0], at(0, -1)),
        remote(x1.at[0, 2 * PART : 3 * PART], above.at[nwin, :PART], lsend.at[1], erecv.at[1], at(1, -1)),
    ]

    spans = [(k * group, group) for k in range(chunks - 1, 0, -1)] + [(0, cut), (cut, group - cut)]

    def back(i):
        start, size = spans[i]
        return remote(
            yr.at[pl.ds(start, size)], yt.at[pl.ds(start + 1, size)], in_sem.at[i], orecv.at[i], at(-1, 0)
        )

    fringe = [
        remote(yo.at[nwin, PART :], yo.at[0, PART :], in_sem.at[chunks + 1], frecv.at[0], at(0, 1)),
        remote(yr.at[nwin - 1, PART :], yt.at[0, PART :], in_sem.at[chunks + 2], frecv.at[1], at(-1, 1)),
    ]

    def bring(b, pieces):
        for i in pieces:
            for d in range(1, n):
                direct[d, b, i].wait_recv()
                for e in range(len(shares[b][2])):
                    if (d, b, i, e) in relays:
                        relays[d, b, i, e].start()

    def settle(b, pieces):
        for (_, r, i, _), c in relays.items():
            if r == b and i in pieces:
                c.wait_recv()

    def windows(pairs, ids):
        return sum([list(range(pairs[i][0], sum(pairs[i]))) for i in ids], [])

    def gather(ref, ws):
        return jnp.concatenate([ref[w] for w in ws], axis=0)

    def block0(parts):
        st = {}
        parts = [(windows(heads_of, ids), ids) for ids in parts]
        ws = sum([p for p, _ in parts], [])

        def wait():
            pass

        def score():
            st["triple"] = project(gather(nq, ws), 0)
            st["scores"] = scores_of(st["triple"], hmask, heads)

        def soften():
            st["att"] = blend(weigh(st["scores"], bias[0], None), st["triple"], hmask, heads)

        def middle():
            st["mid"] = mix(gather(xq, ws).astype(f32), jnp.concatenate(st["att"], axis=0), 0)

        def expand():
            st["hidden"] = widen(st["mid"][1], 0)

        def close():
            mid = st["mid"][0]
            if "hidden" not in st:
                expand()
            start = 0
            for p, ids in parts:
                end = start + len(p) * KEYS
                y = narrow(mid[start:end], st["hidden"][start:end], 0)
                for g, w in enumerate(p):
                    x1[w] = y[g * KEYS : (g + 1) * KEYS]
                start = end
                for i in ids:
                    halo(i).start()
                if 0 in p:
                    for c in edges:
                        c.start()

        return {
            "wait": wait, "score": score, "soften": soften, "middle": middle, "expand": expand, "close": close,
        }

    def own_half(ws):
        return sum([[x1[w, PART : 2 * PART], x1[w + 1, :PART]] for w in ws], [])

    def far_half(ws):
        return sum([[above[w, PART :], above[w + 1, :PART]] for w in ws], [])

    def masks(ws):
        return [jnp.broadcast_to(rt[:, w : w + 1], (KEYS, 128)) == ru[w : w + 1, :] for w in ws]

    def split_rows(x):
        return [x[i : i + 2 * PART] for i in range(0, x.shape[0], 2 * PART)]

    def block1(parts, halos):
        st = {}
        parts = [(windows(spans, ids), ids) for ids in parts]
        ws = sum([p for p, _ in parts], [])

        def wait():
            for c in halos:
                c.wait_recv()

        def score():
            mine, other = own_half(ws), far_half(ws)
            toks = []
            for g in range(0, 2 * len(ws), 2):
                toks += other[g : g + 2] + mine[g : g + 2]
            toks = jnp.concatenate(toks, axis=0).astype(f32)
            st["triple"] = project(layer_norm(toks, gain[1, 0:1], shift[1, 0:1]), 1)
            st["scores"] = scores_of(st["triple"], hmask, heads)

        def soften():
            outs = blend(weigh(st["scores"], bias[1], masks(ws)), st["triple"], hmask, heads)
            st["att"] = [o[: 2 * PART] for o in outs]
            for w, o in zip(ws, outs):
                att[w] = o[2 * PART :]

        def middle():
            x, y = far_half(ws), list(st["att"])
            if nwin - 1 in ws:
                x, y = x + own_half([nwin - 1]), y + [att[nwin - 1]]
            st["mid"] = mix(jnp.concatenate(x, axis=0).astype(f32), jnp.concatenate(y, axis=0), 1)

        def close():
            mid, normed = st["mid"]
            start = 0
            for p, ids in parts:
                tail = nwin - 1 in p
                end = start + (len(p) + tail) * 2 * PART
                ys = split_rows(feed(mid[start:end], normed[start:end], 1))
                for w, y in zip(p, ys):
                    yr[w] = y
                if tail:
                    yo[nwin] = ys[-1]
                start = end
                for i in ids:
                    back(i).start()
                if tail:
                    for c in fringe:
                        c.start()

        return {"wait": wait, "score": score, "soften": soften, "middle": middle, "close": close}

    def own(ws):
        x = jnp.concatenate(own_half(ws), axis=0).astype(f32)
        for w, y in zip(ws, split_rows(feed(*mix(x, gather(att, ws), 1), 1))):
            yo[w + 1] = y

    first = [block0([[0, 1], [2]])] + [block0([[i]]) for i in range(3, len(heads_of))]
    bring(0, (0,))
    settle(0, (0,))
    first[0]["score"]()
    bring(0, (1, 2))
    first[0]["soften"]()
    bring(0, (3,))
    first[0]["middle"]()
    settle(0, (2,))
    first[0]["expand"]()
    first[1]["score"]()
    for c in labels:
        c.wait_send()
    settle(0, (3,))
    first[0]["close"]()
    bring(1, range(4))
    first[1]["soften"]()
    for t in range(1, chunks):
        overlap(first[t + 1] if t < chunks - 1 else None, first[t])
    regions()
    settle(1, range(4))
    second = [block1([[0]], [halo(1), halo(2)] + edges)]
    second += [block1([[i]], [halo(i + 2)]) for i in range(1, chunks - 1)]
    second += [block1([[chunks - 1], [chunks]], [halo(0), halo(chunks + 1)])]
    overlap(second[0], None)
    pl.semaphore_wait(ready, 2)
    for c in smalls + [c for (_, b, _), c in direct.items() if b == 0]:
        c.wait_send()
    own(list(range(final, nwin - 1)))
    for t in range(1, chunks):
        overlap(second[t], second[t - 1])
    overlap(None, second[-1])
    half = nwin // 2
    own(list(range(final)))

    def place(src, base):
        v = src[...].astype(f32)
        for i in range(2):
            left, right = v[:nwin, PART + i * WIN : PART + (i + 1) * WIN], v[1:, i * WIN : (i + 1) * WIN]
            for r, y in enumerate(swap_halves(left, right)):
                o_ref[base + 2 * i + r] = y.reshape(cols, width).astype(bf16)

    fringe[0].wait_recv()
    place(yo, 0)
    for c in edges + fringe + [c for (_, b, _), c in direct.items() if b] + list(relays.values()):
        c.wait_send()
    for i in range(len(heads_of)):
        halo(i).wait_send()
    for i in range(len(spans)):
        back(i).wait_send()
    for i in range(len(spans)):
        back(i).wait_recv()
    fringe[1].wait_recv()
    place(yt, SHIFT)


def on_device(*args):
    x = args[0]
    rows, cols, width = x.shape
    n = lax.axis_size("ch")
    heads = args[7].shape[2] * n
    args = list(args)
    args[5] = args[5].swapaxes(2, 3)
    args[6] = args[6].swapaxes(0, 1)
    args[7] = args[7].swapaxes(1, 2)
    hidden = args[10].shape[2] * n
    nwin = cols // WIN
    group = max(d for d in range(1, MOST + 1) if nwin % d == 0)
    chunks = nwin // group
    assert rows == WIN and heads % 2 == 0 and chunks > 1
    dma = pltpu.SemaphoreType.DMA
    vm = pltpu.VMEM
    scratch = [
        vm(x.shape, bf16), vm((rows, cols), i32), vm(args[2].shape, i32), vm(args[3].shape, f32),
        vm(args[4].shape, f32), vm(args[9].shape, f32), vm(args[13].shape, f32),
        vm((BLOCKS, 3, width, width), bf16), vm((BLOCKS, width, width), bf16),
        vm((BLOCKS, width, hidden), bf16), vm((BLOCKS, hidden, width), bf16),
        vm((n,) + args[7].shape, f32), vm((n,) + args[6].shape, f32), vm((n,) + args[11].shape, f32),
        vm((BLOCKS, 1, 3 * width), f32), vm((BLOCKS, 1, hidden), f32), vm((BLOCKS, KEYS, heads * KEYS), f32),
        vm((3, rows, cols), i32), vm((KEYS, 128), f32), vm((128, 128), f32),
        vm((nwin, KEYS, width), bf16), vm((nwin, KEYS, width), bf16), vm((nwin, 2 * PART, width), bf16),
        vm((nwin + 1, KEYS, width), bf16), vm((nwin + 1, 2 * PART, width), bf16),
        vm((nwin, 2 * PART, width), bf16), vm((nwin + 1, 2 * PART, width), bf16),
        vm((nwin + 1, 2 * PART, width), bf16),
        dma((10 + max(4, chunks),)), dma((max(1, 7 * (n - 2)),)), dma((n - 1, 3)), dma((n - 1, 4)), dma((n - 1, BLOCKS, 4)),
        dma((n - 1, BLOCKS, 4)), dma((n - 1, BLOCKS, 4)), dma((3,)), dma((3,)),
        dma((chunks + 2,)), dma((2,)), dma((chunks + 1,)), dma((2,)),
        pltpu.SemaphoreType.REGULAR,
    ]
    return pl.pallas_call(
        functools.partial(fused, heads, group),
        out_shape=vm(x.shape, bf16),
        in_specs=[pl.BlockSpec(memory_space=pl.ANY)] * len(args),
        out_specs=pl.BlockSpec(memory_space=vm),
        scratch_shapes=scratch,
        compiler_params=pltpu.CompilerParams(
            collective_id=0, has_side_effects=True, vmem_limit_bytes=56 * 1024 * 1024
        ),
        name="fused",
    )(*args)


def solution(mesh):
    in_specs = (
        P(("row", "ch"), "col", None), P(("row", "ch"), "col"), P(), P(), P(),
        P(None, None, None, "ch"), P(None, None, "ch"), P(None, None, "ch"), P(None, "ch", None), P(),
        P(None, None, "ch"), P(None, "ch"), P(None, "ch", None), P(),
    )
    out_specs = P(("row", "ch"), "col", None)
    return jax.shard_map(on_device, mesh=mesh, in_specs=in_specs, out_specs=out_specs, check_vma=False)
```
